256 devices in a mesh: users: 64 (over z, y, x_hi), cols: 4 (over x_lo, core).
Axes of the slice: x: 4 (x_hi: 2, x_lo: 2; x = x_hi * 2 + x_lo), y: 4, z: 8, core: 2. Of those that a mesh axis runs over, the one named last changes fastest.
Arguments:
- item_ids: int32 [1024, 256], P('users'), may hold values from 0 to 131071, as said below
- lengths: int32 [1024], P('users'), may hold values from 1 to 256, 163840 in all
- seed_rows: int32 [1024, 256], P('users'), may hold values from 0 to 63
- item_table: bfloat16 [131072, 1024], P('users', 'cols'), may hold values from -0.59765625 to 0.59765625
- bilinear: bfloat16 [1024, 1024], P(None, 'cols'), may hold values from -0.1875 to 0.1875
- seed_table: float32 [64, 8], replicated, may hold values from -260 to 260
Outputs:
- capsules: float32 [1024, 8, 1024], P('users', None, 'cols')
The draws below stay inside these ranges and needn't reach their ends.
Inputs may be any that keep to these rules, and one draw needn't show every extreme that they name: `item_ids`: ids 2048 * s to 2048 * (s + 1) - 1 form table shard s. Of the 4096 ids of one index of users, at most 128 lie in one shard, and exactly 128 lie in some shard.
All inputs are finite; a program needn't handle non-finite values. No bound on the sum of `lengths` on one device may be relied on, other than what follows from the above.
Results may differ from the reference program's by a relative error of at most 0.0046.
Values may be sent and summed in bfloat16 or wider, within the bound.
A program may use at most 128 MiB of HBM per device.

```python
import math
import jax
import jax.numpy as jnp
import numpy as np
from jax import lax

D = 1024
K = 8
HIST = 256
ITERS = 3
SEEDS = 64
U_DEV = 16
ROWS_DEV = 2048
USERS = 1024
VOCAB = 131072
CAP = 128


def draw_item_ids(key, part):
    blocks = USERS // U_DEV
    tok_count = U_DEV * HIST
    owners = VOCAB // ROWS_DEV

    def draw_block(block_index):
        block_key = jax.random.fold_in(key, block_index)
        key_perm, key_hot, key_mix, key_rows = jax.random.split(block_key, 4)
        shuffled = jax.random.permutation(key_perm, owners * CAP)
        hot_owner = jax.random.randint(key_hot, (), 0, owners)
        priority = jnp.where(shuffled // CAP == hot_owner, 0, 1).astype(jnp.int32)
        ranking = jnp.argsort(priority, stable=True)
        chosen = shuffled[ranking][:tok_count]
        chosen = chosen[jax.random.permutation(key_mix, tok_count)]
        row_in = jax.random.randint(key_rows, (tok_count,), 0, ROWS_DEV)
        return (chosen // CAP * ROWS_DEV + row_in).astype(jnp.int32)
    return jax.vmap(draw_block)(jnp.arange(blocks)).reshape(USERS, HIST)


def draw_seed_table(key, part):
    key_base = jax.random.fold_in(jax.random.fold_in(key, 7), 0)
    return 1.5 * jax.random.normal(key_base, (SEEDS, K), jnp.float32)


def set_ends(values, own_key, least, high):
    shape = values.shape
    place = [jax.random.randint(jax.random.fold_in(own_key, axis), (), 0, shape[axis]) for axis in range(len(shape))]
    values = values.at[tuple(place)].set(least)
    longest = shape.index(max(shape))
    place[longest] = (place[longest] + 1) % shape[longest]
    return values.at[tuple(place)].set(high)


def block_scale(rng, shape, cuts, smallest, top_value):
    def one(axis_at, shards_of):
        steps = jax.random.uniform(jax.random.fold_in(jax.random.fold_in(rng, 6), axis_at), (shards_of,), jnp.float32, smallest / len(cuts), top_value / len(cuts))
        return jnp.repeat(jnp.exp(steps), shape[axis_at] // shards_of).reshape((-1,) + (1,) * (len(shape) - axis_at - 1))

    loudness = one(*cuts[0])
    for cut in cuts[1:]:
        loudness = loudness * one(*cut)
    return loudness


def length_profile(count, total, limit, lean):
    portions = [(1 << 20) // math.isqrt(standing ** lean) + 1 for standing in range(2, count + 1)]
    rest, counts = total - limit - (count - 1), [1] * (count - 1)
    while rest > 0:
        movable = [i for i in range(count - 1) if counts[i] < limit]
        whole, budget = sum([portions[i] for i in movable]), rest
        for i in movable:
            addition = min(limit - counts[i], max(1, budget * portions[i] // whole), rest)
            counts[i] = counts[i] + addition
            rest = rest - addition
    return np.array([limit] + counts)


def ragged_sizes(rng, amount, total, bound, skew):
    if amount == 2:
        one = jax.random.randint(rng, (), max(1, total - bound), min(bound, total - 1) + 1)
        return jnp.stack([one, total - one])
    sizes = jnp.asarray(length_profile(amount, total, bound, skew), jnp.int32)
    pairs = (amount - 1) // 2
    source_of, receiver = sizes[1:1 + 2 * pairs:2], sizes[2:2 + 2 * pairs:2]
    margin = jnp.minimum(source_of - 1, bound - receiver)
    moved = jax.random.randint(jax.random.fold_in(rng, 1), (pairs,), 0, 1 << 20) % (margin + 1)
    sizes = sizes.at[1:1 + 2 * pairs:2].set(source_of - moved).at[2:2 + 2 * pairs:2].set(receiver + moved)
    return sizes[jax.random.permutation(jax.random.fold_in(rng, 2), amount)]


def normal_values(rng, dims, scale, limit, pieces=(), kind=jnp.bfloat16):
    values = jax.random.normal(rng, dims, jnp.float32) * scale
    if len(pieces) > 0:
        values = block_scale(rng, dims, pieces, -0.22, 0.18) * values
    return jnp.clip(values, min=-limit, max=limit).astype(kind)


def setup_inputs(seed: int = 0) -> dict:
    key_of = jax.random.split(jax.random.key(seed), 7)
    return {
        "item_ids": draw_item_ids(jax.random.fold_in(key_of[6], 71), 0),
        "lengths": ragged_sizes(key_of[1], USERS, USERS * HIST * 5 // 8, HIST, 2).astype(jnp.int32),
        "seed_rows": set_ends(jax.random.randint(key_of[2], (USERS, HIST), 0, SEEDS), jax.random.fold_in(key_of[2], 1), 0, SEEDS - 1).astype(jnp.int32),
        "item_table": normal_values(key_of[3], (VOCAB, D), 0.1, 0.59765625, ((0, 64), (1, 4))),
        "bilinear": normal_values(key_of[4], (D, D), D ** -0.5, 0.1875, ((1, 4),)),
        "seed_table": draw_seed_table(jax.random.fold_in(key_of[6], 71), 0),
    }


def squash_scale(squares):
    return squares / (1.0 + squares) / jnp.sqrt(squares + 1e-06)

def reference(item_ids, lengths, seed_rows, item_table, bilinear, seed_table):
    blocks = USERS // U_DEV

    def per_block(inputs):
        block_ids, block_seeds, block_lens = inputs
        embedded = item_table[block_ids.reshape(-1)]
        mapped = jnp.dot(embedded, bilinear, preferred_element_type=jnp.float32).astype(jnp.bfloat16)
        mapped = lax.optimization_barrier(mapped).astype(jnp.float32).reshape(U_DEV, HIST, D)
        logits = seed_table[block_seeds]
        position = jnp.arange(HIST, dtype=jnp.int32)
        live = (position[None, :] < block_lens[:, None]).astype(jnp.float32)
        capsules = jnp.zeros((U_DEV, K, D), jnp.float32)
        for step in range(ITERS):
            weights = (jax.nn.softmax(logits, axis=-1) * live[:, :, None]).astype(jnp.bfloat16)
            weights = lax.optimization_barrier(weights).astype(jnp.float32)
            summed = jnp.einsum('utk,utd->ukd', weights, mapped, precision=lax.Precision.HIGHEST)
            squares = lax.optimization_barrier(jnp.sum(summed * summed, axis=-1))
            capsules = summed * squash_scale(squares)[:, :, None]
            if step + 1 < ITERS:
                logits = logits + jnp.einsum('utd,ukd->utk', mapped, capsules, precision=lax.Precision.HIGHEST)
        return capsules
    result = lax.map(per_block, (item_ids.reshape(blocks, U_DEV, HIST), seed_rows.reshape(blocks, U_DEV, HIST), lengths.reshape(blocks, U_DEV)))
    return result.reshape(USERS, K, D)
```

```python
import functools

import jax
import jax.numpy as jnp
from jax import lax
from jax.experimental import pallas as pl
from jax.experimental.pallas import tpu as pltpu
from jax.sharding import PartitionSpec as P

ITERS = 3
GROUPS = 64
COLS = 4
LANES = 128
BATCH = 8
CHUNKS = 4
MESH = pl.DeviceIdType.MESH
BF16 = jnp.bfloat16
F32 = jnp.float32
NT = (((1,), (1,)), ((), ()))


def squash_scale(squares):
    return squares / (1.0 + squares) / jnp.sqrt(squares + 1e-06)


def split_two(value):
    high = value.astype(BF16)
    low = (value - high.astype(F32)).astype(BF16)
    return high, low


def softmax_rows(logits):
    shifted = jnp.exp(logits - jnp.max(logits, axis=0, keepdims=True))
    return (shifted / jnp.sum(shifted, axis=0, keepdims=True)).astype(BF16)


def kernel(
    cap,
    ids_ref, len_ref, seed_ref, table_ref, map_ref, seed_table_ref,
    out_ref,
    req_out, req_in, users_of, seeds_of, gathered, mapped, send_rows, rows,
    logits, weights, agree_out, agree_in, square_out, square_in,
    req_send, req_recv, tab_send, tab_recv, relay_send, relay_recv,
    row_send, row_recv, cols_send, cols_recv, sq_send, sq_recv,
):
    me = lax.axis_index("users")
    col = lax.axis_index("cols")
    users, hist = ids_ref.shape
    rows_dev = table_ref.shape[0]
    half = table_ref.shape[1]
    capsules = seed_table_ref.shape[1]
    pairs = users * capsules
    tiles = GROUPS * cap // LANES
    per_tile = LANES // cap
    chunk = rows_dev // CHUNKS
    partner = col + 1 - 2 * lax.rem(col, 2)
    cross = lax.rem(col + 2, COLS)
    diagonal = lax.rem(partner + 2, COLS)

    def group_at(step):
        return lax.rem(me + step, GROUPS)

    barrier = pltpu.get_barrier_semaphore()

    @pl.loop(1, GROUPS)
    def _(step):
        pl.semaphore_signal(barrier, inc=1, device_id={"users": group_at(step)}, device_id_type=MESH)

    for other in (partner, cross, diagonal):
        pl.semaphore_signal(barrier, inc=1, device_id={"cols": other}, device_id_type=MESH)

    position = lax.broadcasted_iota(jnp.int32, (1, hist), 1)
    owner_iota = lax.broadcasted_iota(jnp.int32, (GROUPS, hist), 0)
    tile_iota = lax.broadcasted_iota(jnp.int32, (tiles, hist), 0)
    rank_iota = lax.broadcasted_iota(jnp.int32, (LANES, hist), 0)
    upper = (
        lax.broadcasted_iota(jnp.int32, (hist, hist), 0)
        <= lax.broadcasted_iota(jnp.int32, (hist, hist), 1)
    ).astype(F32).astype(BF16)
    ones = jnp.ones((hist, hist), BF16)
    tri = jnp.concatenate([upper, ones], axis=0)
    before = jnp.zeros((GROUPS, hist), F32)
    requests = jnp.zeros((2 * GROUPS, LANES), F32)
    meta = jnp.zeros((2 * tiles, LANES), F32)
    for user in range(users):
        ids = ids_ref[user : user + 1, :]
        owner = ids // rows_dev
        row = ids - owner * rows_dev
        live = position < len_ref[user]
        owner = jnp.where(live, owner, -1)
        onehot = jnp.where(owner_iota == owner, 1.0, 0.0)
        both = jnp.concatenate([onehot.astype(BF16), before.astype(BF16)], axis=1)
        counts = jnp.dot(both, tri, preferred_element_type=F32)
        before = before + onehot
        rank = (jnp.sum(counts * onehot, axis=0, keepdims=True) - 1.0).astype(jnp.int32)
        high = (row // 256).astype(F32) + 8.0
        low = (row - row // 256 * 256).astype(F32)
        left = jnp.concatenate([(onehot * high).astype(BF16), (onehot * low).astype(BF16)], axis=0)
        at_rank = jnp.where(rank_iota == rank, 1.0, 0.0).astype(BF16)
        requests = requests + lax.dot_general(left, at_rank, NT, preferred_element_type=F32)
        tile = jnp.where(rank < cap, owner // per_tile, -1)
        place = rank + (owner - owner // per_tile * per_tile) * cap
        onehot_tile = jnp.where(tile_iota == tile, 1.0, 0.0)
        seeds = seed_ref[user : user + 1, :].astype(F32)
        left = jnp.concatenate(
            [(onehot_tile * (user + 1.0)).astype(BF16), (onehot_tile * seeds).astype(BF16)], axis=0
        )
        at_place = jnp.where(rank_iota == place, 1.0, 0.0).astype(BF16)
        meta = meta + lax.dot_general(left, at_place, NT, preferred_element_type=F32)
    asked = (requests[:GROUPS] - 8.0) * 256.0 + requests[GROUPS:]
    asked = jnp.where(requests[:GROUPS] > 0.0, asked, -1.0).astype(jnp.int32)
    for owner in range(GROUPS):
        req_out[owner] = asked[owner : owner + 1, :]
    user_ids = meta[:tiles].astype(jnp.int32) - 1
    seed_ids = meta[tiles:].astype(jnp.int32)
    for tile in range(tiles):
        users_of[tile] = jnp.broadcast_to(user_ids[tile : tile + 1, :], (8, LANES))
        seeds_of[tile] = jnp.broadcast_to(seed_ids[tile : tile + 1, :], (8, LANES))

    pl.semaphore_wait(barrier, GROUPS - 1 + COLS - 1)

    def table_copy(part, target, slot):
        return pltpu.make_async_remote_copy(
            src_ref=table_ref.at[pl.ds(part * chunk, chunk)],
            dst_ref=gathered.at[col, pl.ds(part * chunk, chunk)],
            send_sem=tab_send.at[slot, part],
            recv_sem=tab_recv.at[slot, part],
            device_id={"cols": target},
            device_id_type=MESH,
        )

    def relay_copy(part):
        return pltpu.make_async_remote_copy(
            src_ref=gathered.at[cross, pl.ds(part * chunk, chunk)],
            dst_ref=gathered.at[cross, pl.ds(part * chunk, chunk)],
            send_sem=relay_send.at[part],
            recv_sem=relay_recv.at[part],
            device_id={"cols": partner},
            device_id_type=MESH,
        )

    for part in range(CHUNKS):
        table_copy(part, cross, 0).start()
    for part in range(CHUNKS):
        table_copy(part, partner, 1).start()

    def request_copy(target, landing):
        return pltpu.make_async_remote_copy(
            src_ref=req_out.at[target],
            dst_ref=req_in.at[landing],
            send_sem=req_send.at[target],
            recv_sem=req_recv.at[landing],
            device_id={"users": target},
            device_id_type=MESH,
        )

    @pl.loop(1, GROUPS)
    def _(step):
        request_copy(group_at(step), me).start()

    req_in[me] = req_out[me]

    seed_table = seed_table_ref[...]
    seed_high, seed_low = split_two(seed_table)
    seed_rest = (seed_table - seed_high.astype(F32) - seed_low.astype(F32)).astype(BF16)
    seed_count = seed_table.shape[0]
    seed_iota = lax.broadcasted_iota(jnp.int32, (seed_count, LANES), 0)

    def store_weights(tile, value):
        picked = users_of[tile]
        routed = softmax_rows(value).astype(F32)
        stacked = jnp.concatenate(
            [jnp.where(picked == user, routed, 0.0) for user in range(users)], axis=0
        )
        weights[tile] = stacked.astype(BF16)

    @pl.loop(0, tiles)
    def _(tile):
        chosen = jnp.where(seed_iota == seeds_of[tile][0:1, :], 1.0, 0.0).astype(BF16)
        start = jnp.zeros((capsules, LANES), F32)
        for part in (seed_rest, seed_low, seed_high):
            start = start + lax.dot_general(
                part, chosen, (((0,), (0,)), ((), ())), preferred_element_type=F32
            )
        logits[tile] = start
        store_weights(tile, start)

    for part in range(CHUNKS):
        table_copy(part, cross, 0).wait_recv()
        relay_copy(part).start()
    for part in range(CHUNKS):
        table_copy(part, partner, 1).wait_recv()
        relay_copy(part).wait_recv()
        span = pl.ds(part * chunk, chunk)
        value = jnp.dot(table_ref[span], map_ref[col], preferred_element_type=F32)
        for source in (partner, cross, diagonal):
            value = value + jnp.dot(gathered[source, span], map_ref[source], preferred_element_type=F32)
        mapped[span] = value.astype(BF16)

    @pl.loop(1, GROUPS)
    def _(step):
        request_copy(group_at(step), group_at(step)).wait_recv()

    def row_copy(target, landing):
        return pltpu.make_async_remote_copy(
            src_ref=send_rows.at[target],
            dst_ref=rows.at[landing],
            send_sem=row_send.at[target],
            recv_sem=row_recv.at[landing],
            device_id={"users": target},
            device_id_type=MESH,
        )

    batches = GROUPS // BATCH
    lane_iota = lax.broadcasted_iota(jnp.int32, (cap, rows_dev), 1)

    @pl.loop(0, batches)
    def _(batch):
        wanted = jnp.concatenate(
            [req_in[group_at(batch + batches * item)] for item in range(BATCH)], axis=0
        )
        columns = wanted.astype(F32).T.astype(jnp.int32)
        onehot = jnp.concatenate(
            [
                jnp.where(lane_iota == columns[:cap, item : item + 1], 1.0, 0.0).astype(BF16)
                for item in range(BATCH)
            ],
            axis=0,
        )
        served = jnp.dot(onehot, mapped[...], preferred_element_type=F32).astype(BF16)
        for item in range(BATCH):
            send_rows[group_at(batch + batches * item)] = served[item * cap : (item + 1) * cap]
        for item in range(BATCH):
            if item:
                row_copy(group_at(batch + batches * item), me).start()
            else:

                @pl.when(batch > 0)
                def _():
                    row_copy(group_at(batch), me).start()

    rows[me] = send_rows[me]

    @pl.loop(1, GROUPS)
    def _(step):
        row_copy(group_at(step), group_at(step)).wait_recv()

    def cols_copy(step, hop, target):
        source = agree_out.at[step] if hop == 0 else agree_out.at[2 + step]
        return pltpu.make_async_remote_copy(
            src_ref=source,
            dst_ref=agree_in.at[2 * step + hop],
            send_sem=cols_send.at[2 * step + hop],
            recv_sem=cols_recv.at[2 * step + hop],
            device_id={"cols": target},
            device_id_type=MESH,
        )

    lane_of = lax.broadcasted_iota(jnp.int32, (8, LANES), 1)
    per_source = cap // LANES if cap > LANES else 1
    del per_source

    def tile_rows(tile):
        if per_tile == 1:
            return rows[tile]
        return jnp.concatenate([rows[tile * per_tile + k] for k in range(per_tile)], axis=0)

    for step in range(ITERS):
        summed = lax.fori_loop(
            0,
            tiles // 2,
            lambda i, acc: acc
            + jnp.dot(
                jnp.concatenate([weights[2 * i], weights[2 * i + 1]], axis=1),
                jnp.concatenate([tile_rows(2 * i), tile_rows(2 * i + 1)], axis=0),
                preferred_element_type=F32,
            ),
            jnp.zeros((pairs, half), F32),
        )
        partial = jnp.sum(summed * summed, axis=1, keepdims=True)
        packed = jnp.zeros((8, LANES), F32)
        for user in range(users):
            packed = jnp.where(lane_of == user, partial[user * 8 : user * 8 + 8], packed)
        if step + 1 < ITERS:
            parts = jnp.concatenate(split_two(summed), axis=0)

            @pl.loop(0, tiles // 2)
            def _(i):
                landed = jnp.concatenate([tile_rows(2 * i), tile_rows(2 * i + 1)], axis=0)
                product = lax.dot_general(parts, landed, NT, preferred_element_type=F32)
                product = product[:pairs] + product[pairs:]
                for k in range(2):
                    picked = users_of[2 * i + k]
                    own = jnp.zeros((8, LANES), F32)
                    for user in range(users):
                        piece = product[user * 8 : user * 8 + 8, k * LANES : (k + 1) * LANES]
                        own = jnp.where(picked == user, piece, own)
                    agree_out[step, 2 * i + k] = own

            agree_out[step, tiles] = packed
            cols_copy(step, 0, partner).start()
            cols_copy(step, 0, partner).wait_recv()
            agree_out[2 + step] = agree_out[step] + agree_in[2 * step]
            cols_copy(step, 1, cross).start()
            cols_copy(step, 1, cross).wait_recv()
            squares = agree_out[2 + step, tiles] + agree_in[2 * step + 1, tiles]
            scale = squash_scale(squares)
            scales = [jnp.broadcast_to(scale[:, user : user + 1], (8, LANES)) for user in range(users)]

            @pl.loop(0, tiles)
            def _(tile):
                picked = users_of[tile]
                factor = jnp.zeros((8, LANES), F32)
                for user in range(users):
                    factor = jnp.where(picked == user, scales[user], factor)
                total = agree_out[2 + step, tile] + agree_in[2 * step + 1, tile]
                value = logits[tile] + factor * total
                logits[tile] = value
                store_weights(tile, value)

        else:
            square_out[...] = packed
            copies = []
            for slot, target in enumerate((partner, cross, diagonal)):
                copies.append(
                    pltpu.make_async_remote_copy(
                        src_ref=square_out,
                        dst_ref=square_in.at[slot],
                        send_sem=sq_send.at[slot],
                        recv_sem=sq_recv.at[slot],
                        device_id={"cols": target},
                        device_id_type=MESH,
                    )
                )
            for copy in copies:
                copy.start()
            for copy in copies:
                copy.wait_recv()
            squares = (square_out[...] + square_in[0]) + (square_in[1] + square_in[2])
            scale = squash_scale(squares)
            for user in range(users):
                out_ref[user] = summed[user * 8 : user * 8 + 8] * scale[:, user : user + 1]
            for copy in copies:
                copy.wait_send()

    for part in range(CHUNKS):
        table_copy(part, cross, 0).wait_send()
        table_copy(part, partner, 1).wait_send()
        relay_copy(part).wait_send()

    @pl.loop(1, GROUPS)
    def _(step):
        request_copy(group_at(step), me).wait_send()
        row_copy(group_at(step), me).wait_send()

    for step in range(ITERS - 1):
        cols_copy(step, 0, partner).wait_send()
        cols_copy(step, 1, cross).wait_send()


def on_device(cap, item_ids, lengths, seed_rows, item_table, bilinear, seed_table):
    users, hist = item_ids.shape
    rows_dev, half = item_table.shape
    capsules = seed_table.shape[1]
    tiles = GROUPS * cap // LANES
    vmem = pl.BlockSpec(memory_space=pltpu.VMEM)
    dma = pltpu.SemaphoreType.DMA
    return pl.pallas_call(
        functools.partial(kernel, cap),
        out_shape=jax.ShapeDtypeStruct((users, capsules, half), F32),
        in_specs=[vmem, pl.BlockSpec(memory_space=pltpu.SMEM), vmem, vmem, vmem, vmem],
        out_specs=vmem,
        scratch_shapes=[
            pltpu.VMEM((GROUPS, 1, LANES), jnp.int32),
            pltpu.VMEM((GROUPS, 1, LANES), jnp.int32),
            pltpu.VMEM((tiles, 8, LANES), jnp.int32),
            pltpu.VMEM((tiles, 8, LANES), jnp.int32),
            pltpu.VMEM((COLS, rows_dev, half), BF16),
            pltpu.VMEM((rows_dev, half), BF16),
            pltpu.VMEM((GROUPS, cap, half), BF16),
            pltpu.VMEM((GROUPS, cap, half), BF16),
            pltpu.VMEM((tiles, 8, LANES), F32),
            pltpu.VMEM((tiles, users * capsules, LANES), BF16),
            pltpu.VMEM((4, tiles + 1, 8, LANES), F32),
            pltpu.VMEM((4, tiles + 1, 8, LANES), F32),
            pltpu.VMEM((8, LANES), F32),
            pltpu.VMEM((3, 8, LANES), F32),
            dma((GROUPS,)), dma((GROUPS,)),
            dma((2, CHUNKS)), dma((2, CHUNKS)), dma((CHUNKS,)), dma((CHUNKS,)),
            dma((GROUPS,)), dma((GROUPS,)),
            dma((4,)), dma((4,)), dma((3,)), dma((3,)),
        ],
        compiler_params=pltpu.CompilerParams(
            collective_id=0, has_side_effects=True, vmem_limit_bytes=56 << 20
        ),
    )(item_ids, lengths, seed_rows, item_table, bilinear.reshape(COLS, -1, half), seed_table)


def solution(mesh):
    placed = (
        P("users", None),
        P("users"),
        P("users", None),
        P("users", "cols"),
        P(None, "cols"),
        P(),
    )
    return jax.shard_map(
        functools.partial(on_device, 128),
        mesh=mesh,
        in_specs=placed,
        out_specs=P("users", None, "cols"),
        check_vma=False,
    )
```

```python
import functools

import jax
import jax.numpy as jnp
from jax import lax
from jax.experimental import pallas as pl
from jax.experimental.pallas import tpu as pltpu
from jax.sharding import PartitionSpec as P

ITERS = 3
GROUPS = 64
COLS = 4
LANES = 128
BATCH = 8
CHUNKS = 4
HOP = 8
SPILL = 2
MESH = pl.DeviceIdType.MESH
BF16 = jnp.bfloat16
F32 = jnp.float32
NT = (((1,), (1,)), ((), ()))


def squash_scale(squares):
    return squares / (1.0 + squares) / jnp.sqrt(squares + 1e-06)


def split_two(value):
    high = value.astype(BF16)
    low = (value - high.astype(F32)).astype(BF16)
    return high, low


def softmax_rows(logits):
    shifted = jnp.exp(logits - jnp.max(logits, axis=0, keepdims=True))
    return (shifted / jnp.sum(shifted, axis=0, keepdims=True)).astype(BF16)


def kernel(
    cap,
    ids_ref, len_ref, seed_ref, table_ref, map_ref, seed_table_ref,
    out_ref, fail_ref,
    req_out, req_in, users_of, seeds_of, gathered, mapped, send_rows, rows,
    logits, weights, agree_out, agree_in, square_out, square_in,
    ask_out, ask_in, relay_rows_out, relay_rows_in, relay_stage, spill_out, spill_in, spill_stage,
    req_send, req_recv, tab_send, tab_recv, relay_send, relay_recv,
    row_send, row_recv, cols_send, cols_recv, sq_send, sq_recv,
    ask_send, ask_recv, hop_send, hop_recv, spill_send, spill_recv,
):
    me = lax.axis_index("users")
    col = lax.axis_index("cols")
    users, hist = ids_ref.shape
    rows_dev = table_ref.shape[0]
    half = table_ref.shape[1]
    capsules = seed_table_ref.shape[1]
    pairs = users * capsules
    relayed = cap < LANES
    main_tiles = GROUPS * cap // LANES
    tiles = main_tiles + (1 if relayed else 0)
    per_tile = LANES // cap
    chunk = rows_dev // CHUNKS
    partner = col + 1 - 2 * lax.rem(col, 2)
    cross = lax.rem(col + 2, COLS)
    diagonal = lax.rem(partner + 2, COLS)

    def group_at(step):
        return lax.rem(me + step, GROUPS)

    barrier = pltpu.get_barrier_semaphore()

    @pl.loop(1, GROUPS)
    def _(step):
        pl.semaphore_signal(barrier, inc=1, device_id={"users": group_at(step)}, device_id_type=MESH)

    for other in (partner, cross, diagonal):
        pl.semaphore_signal(barrier, inc=1, device_id={"cols": other}, device_id_type=MESH)

    position = lax.broadcasted_iota(jnp.int32, (1, hist), 1)
    owner_iota = lax.broadcasted_iota(jnp.int32, (GROUPS, hist), 0)
    tile_iota = lax.broadcasted_iota(jnp.int32, (tiles, hist), 0)
    rank_iota = lax.broadcasted_iota(jnp.int32, (LANES, hist), 0)
    upper = (
        lax.broadcasted_iota(jnp.int32, (hist, hist), 0)
        <= lax.broadcasted_iota(jnp.int32, (hist, hist), 1)
    ).astype(F32).astype(BF16)
    ones = jnp.ones((hist, hist), BF16)
    tri = jnp.concatenate([upper, ones], axis=0)
    before = jnp.zeros((GROUPS, hist), F32)
    owners, in_rows, ranks = [], [], []
    for user in range(users):
        ids = ids_ref[user : user + 1, :]
        owner = ids // rows_dev
        in_rows.append(ids - owner * rows_dev)
        owner = jnp.where(position < len_ref[user], owner, -1)
        owners.append(owner)
        onehot = jnp.where(owner_iota == owner, 1.0, 0.0)
        both = jnp.concatenate([onehot.astype(BF16), before.astype(BF16)], axis=1)
        counts = jnp.dot(both, tri, preferred_element_type=F32)
        before = before + onehot
        ranks.append((jnp.sum(counts * onehot, axis=0, keepdims=True) - 1.0).astype(jnp.int32))
    if relayed:
        over = [jnp.where(rank >= cap, 1.0, 0.0) for rank in ranks]
        over_rows = jnp.concatenate(over, axis=0)
        over_before = [jnp.zeros((1, hist), F32)]
        for user in range(users):
            over_before.append(over_before[-1] + over[user])
        sums = jnp.concatenate(over_before[:users], axis=0)
        both = jnp.concatenate([over_rows.astype(BF16), sums.astype(BF16)], axis=1)
        queue = (jnp.dot(both, tri, preferred_element_type=F32) - 1.0).astype(jnp.int32)
        over_total = jnp.sum(over_before[users], axis=1, keepdims=True)
    requests = jnp.zeros((3 * GROUPS, LANES), F32)
    meta = jnp.zeros((2 * tiles, LANES), F32)
    for user in range(users):
        owner, row, rank = owners[user], in_rows[user], ranks[user]
        target, place = owner, rank
        tile = owner // per_tile
        spot = rank + (owner - tile * per_tile) * cap
        tile = jnp.where(owner >= 0, tile, -1)
        if relayed:
            line = queue[user : user + 1, :]
            turn = line // GROUPS
            spills = rank >= cap
            fits = turn < SPILL
            relay = lax.rem(line + me * 9, GROUPS)
            target = jnp.where(spills, jnp.where(fits, relay, -1), owner)
            place = jnp.where(spills, cap + turn, rank)
            tile = jnp.where(spills, jnp.where(fits, main_tiles, -1), tile)
            spot = jnp.where(spills, relay * SPILL + turn, spot)
        onehot = jnp.where(owner_iota == target, 1.0, 0.0)
        high = (row // 256).astype(F32) + 8.0
        low = (row - row // 256 * 256).astype(F32)
        left = jnp.concatenate(
            [(onehot * part).astype(BF16) for part in (high, low, owner.astype(F32))], axis=0
        )
        at_place = jnp.where(rank_iota == place, 1.0, 0.0).astype(BF16)
        requests = requests + lax.dot_general(left, at_place, NT, preferred_element_type=F32)
        onehot_tile = jnp.where(tile_iota == tile, 1.0, 0.0)
        seeds = seed_ref[user : user + 1, :].astype(F32)
        left = jnp.concatenate(
            [(onehot_tile * (user + 1.0)).astype(BF16), (onehot_tile * seeds).astype(BF16)], axis=0
        )
        at_spot = jnp.where(rank_iota == spot, 1.0, 0.0).astype(BF16)
        meta = meta + lax.dot_general(left, at_spot, NT, preferred_element_type=F32)
    asked = (requests[:GROUPS] - 8.0) * 256.0 + requests[GROUPS : 2 * GROUPS]
    lane_all = lax.broadcasted_iota(jnp.int32, (GROUPS, LANES), 1)
    if relayed:
        whole = asked + requests[2 * GROUPS :] * float(rows_dev)
        asked = jnp.where(lane_all < cap, asked, whole)
    asked = jnp.where(requests[:GROUPS] > 0.0, asked, -1.0)
    if relayed:
        too_many = jnp.where(over_total > float(SPILL * GROUPS), 1.0, 0.0)
        asked = jnp.where(lane_all == LANES - 1, too_many, asked)
    asked = asked.astype(jnp.int32)
    for owner in range(GROUPS):
        req_out[owner] = asked[owner : owner + 1, :]
    user_ids = meta[:tiles].astype(jnp.int32) - 1
    seed_ids = meta[tiles:].astype(jnp.int32)
    for tile in range(tiles):
        users_of[tile] = jnp.broadcast_to(user_ids[tile : tile + 1, :], (8, LANES))
        seeds_of[tile] = jnp.broadcast_to(seed_ids[tile : tile + 1, :], (8, LANES))

    pl.semaphore_wait(barrier, GROUPS - 1 + COLS - 1)

    def table_copy(part, target, slot):
        return pltpu.make_async_remote_copy(
            src_ref=table_ref.at[pl.ds(part * chunk, chunk)],
            dst_ref=gathered.at[col, pl.ds(part * chunk, chunk)],
            send_sem=tab_send.at[slot, part],
            recv_sem=tab_recv.at[slot, part],
            device_id={"cols": target},
            device_id_type=MESH,
        )

    def relay_copy(part):
        return pltpu.make_async_remote_copy(
            src_ref=gathered.at[cross, pl.ds(part * chunk, chunk)],
            dst_ref=gathered.at[cross, pl.ds(part * chunk, chunk)],
            send_sem=relay_send.at[part],
            recv_sem=relay_recv.at[part],
            device_id={"cols": partner},
            device_id_type=MESH,
        )

    def users_copy(source, landing_in, sends, recvs, target, landing):
        return pltpu.make_async_remote_copy(
            src_ref=source.at[target],
            dst_ref=landing_in.at[landing],
            send_sem=sends.at[target],
            recv_sem=recvs.at[landing],
            device_id={"users": target},
            device_id_type=MESH,
        )

    request_copy = functools.partial(users_copy, req_out, req_in, req_send, req_recv)
    row_copy = functools.partial(users_copy, send_rows, rows, row_send, row_recv)
    ask_copy = functools.partial(users_copy, ask_out, ask_in, ask_send, ask_recv)
    hop_copy = functools.partial(users_copy, relay_rows_out, relay_rows_in, hop_send, hop_recv)
    spill_copy = functools.partial(users_copy, spill_out, spill_in, spill_send, spill_recv)

    def send_all(copy):
        @pl.loop(1, GROUPS)
        def _(step):
            copy(group_at(step), me).start()

    def receive_all(copy):
        @pl.loop(1, GROUPS)
        def _(step):
            copy(group_at(step), group_at(step)).wait_recv()

    send_all(request_copy)
    for part in range(CHUNKS):
        table_copy(part, cross, 0).start()
    for part in range(CHUNKS):
        table_copy(part, partner, 1).start()
    req_in[me] = req_out[me]

    seed_table = seed_table_ref[...]
    seed_high, seed_low = split_two(seed_table)
    seed_rest = (seed_table - seed_high.astype(F32) - seed_low.astype(F32)).astype(BF16)
    seed_count = seed_table.shape[0]
    seed_iota = lax.broadcasted_iota(jnp.int32, (seed_count, LANES), 0)

    def store_weights(tile, value):
        picked = users_of[tile]
        routed = softmax_rows(value).astype(F32)
        stacked = jnp.concatenate(
            [jnp.where(picked == user, routed, 0.0) for user in range(users)], axis=0
        )
        weights[tile] = stacked.astype(BF16)

    def each_tile(body):
        @pl.loop(0, main_tiles // 4)
        def _(i):
            for k in range(4):
                body(4 * i + k)

        if relayed:
            body(main_tiles)

    def first_weights(tile):
        chosen = jnp.where(seed_iota == seeds_of[tile][0:1, :], 1.0, 0.0).astype(BF16)
        start = jnp.zeros((capsules, LANES), F32)
        for part in (seed_rest, seed_low, seed_high):
            start = start + lax.dot_general(
                part, chosen, (((0,), (0,)), ((), ())), preferred_element_type=F32
            )
        logits[tile] = start
        store_weights(tile, start)

    each_tile(first_weights)

    receive_all(request_copy)

    if relayed:
        tokens = GROUPS * SPILL
        token_lane = lax.broadcasted_iota(jnp.int32, (GROUPS, tokens), 1)
        token_row = lax.broadcasted_iota(jnp.int32, (GROUPS, tokens), 0)
        message = jnp.concatenate([req_in[g] for g in range(GROUPS)], axis=0)
        wanted = jnp.zeros((GROUPS, tokens), F32)
        for turn in range(SPILL):
            column = message[:, cap + turn : cap + turn + 1].astype(F32) + 1.0
            wanted = jnp.where(token_lane == token_row * SPILL + turn, column, wanted)
        token = jnp.sum(wanted, axis=0, keepdims=True).astype(jnp.int32) - 1
        owner = token // rows_dev
        row = token - owner * rows_dev
        owner = jnp.where(token >= 0, owner, -1)
        onehot = jnp.where(token_row == owner, 1.0, 0.0)
        counts = jnp.dot(onehot.astype(BF16), upper[:tokens, :tokens], preferred_element_type=F32)
        rank = (jnp.sum(counts * onehot, axis=0, keepdims=True) - 1.0).astype(jnp.int32)
        high = (row // 256).astype(F32) + 8.0
        low = (row - row // 256 * 256).astype(F32)
        left = jnp.concatenate([(onehot * high).astype(BF16), (onehot * low).astype(BF16)], axis=0)
        at_rank = jnp.where(rank_iota[:, :tokens] == rank, 1.0, 0.0).astype(BF16)
        hops = lax.dot_general(left, at_rank, NT, preferred_element_type=F32)
        asked = (hops[:GROUPS] - 8.0) * 256.0 + hops[GROUPS:]
        asked = jnp.where(hops[:GROUPS] > 0.0, asked, -1.0)
        flags = jnp.where(lane_all == LANES - 1, message.astype(F32), 0.0)
        flags = jnp.max(jnp.max(flags, axis=0, keepdims=True), axis=1, keepdims=True)
        deep = jnp.max(rank.astype(F32), axis=1, keepdims=True)
        flags = jnp.maximum(flags, jnp.where(deep >= float(HOP), 1.0, 0.0))
        asked = jnp.where(lane_all == LANES - 1, flags, asked).astype(jnp.int32)
        for target in range(GROUPS):
            ask_out[target] = asked[target : target + 1, :]
        landed_at = jnp.where(owner >= 0, owner * HOP + rank, -1)
        landed_at = jnp.broadcast_to(landed_at, (8, tokens)).astype(F32).T.astype(jnp.int32)[:, 0:1]
        send_all(ask_copy)
        ask_in[me] = ask_out[me]

    for part in range(CHUNKS):
        table_copy(part, cross, 0).wait_recv()
        relay_copy(part).start()
    for part in range(CHUNKS):
        table_copy(part, partner, 1).wait_recv()
        relay_copy(part).wait_recv()
        span = pl.ds(part * chunk, chunk)
        value = jnp.dot(table_ref[span], map_ref[col], preferred_element_type=F32)
        for source in (partner, cross, diagonal):
            value = value + jnp.dot(gathered[source, span], map_ref[source], preferred_element_type=F32)
        mapped[span] = value.astype(BF16)

    if relayed:
        receive_all(ask_copy)
        message = jnp.concatenate([ask_in[g] for g in range(GROUPS)], axis=0).astype(F32)
        flags = jnp.where(lane_all == LANES - 1, message, 0.0)
        flags = jnp.max(jnp.max(flags, axis=0, keepdims=True), axis=1, keepdims=True)
        fail_ref[...] = jnp.broadcast_to(flags, (8, LANES)).astype(jnp.int32)
        columns = message.T.astype(jnp.int32)
        hop_iota = lax.broadcasted_iota(jnp.int32, (HOP, rows_dev), 1)
        onehot = jnp.concatenate(
            [
                jnp.where(hop_iota == columns[:HOP, g : g + 1], 1.0, 0.0)
                for g in range(GROUPS)
            ],
            axis=0,
        ).astype(BF16)
        served = jnp.dot(onehot, mapped[...], preferred_element_type=F32)
        for g in range(GROUPS):
            relay_rows_out[g] = served[g * HOP : (g + 1) * HOP].astype(BF16)
        send_all(hop_copy)
        relay_rows_in[me] = relay_rows_out[me]
    else:
        fail_ref[...] = jnp.zeros((8, LANES), jnp.int32)

    batches = GROUPS // BATCH
    lane_iota = lax.broadcasted_iota(jnp.int32, (cap, rows_dev), 1)

    def serve(batch):
        wanted = jnp.concatenate(
            [req_in[group_at(batch + batches * item)] for item in range(BATCH)], axis=0
        )
        columns = wanted.astype(F32).T.astype(jnp.int32)
        onehot = jnp.concatenate(
            [
                jnp.where(lane_iota == columns[:cap, item : item + 1], 1.0, 0.0).astype(BF16)
                for item in range(BATCH)
            ],
            axis=0,
        )
        served = jnp.dot(onehot, mapped[...], preferred_element_type=F32).astype(BF16)
        for item in range(BATCH):
            send_rows[group_at(batch + batches * item)] = served[item * cap : (item + 1) * cap]
        for item in range(BATCH):
            if item:
                row_copy(group_at(batch + batches * item), me).start()
            else:

                @pl.when(batch > 0)
                def _():
                    row_copy(group_at(batch), me).start()

    early = batches // 2 if relayed else batches

    @pl.loop(0, early)
    def _(batch):
        serve(batch)

    if relayed:
        receive_all(hop_copy)
        for g in range(GROUPS):
            relay_stage[g * HOP : (g + 1) * HOP] = relay_rows_in[g].astype(F32)
        hop_lane = lax.broadcasted_iota(jnp.int32, (tokens, GROUPS * HOP), 1)
        onehot = jnp.where(hop_lane == landed_at, 1.0, 0.0).astype(BF16)
        spilled = jnp.dot(onehot, relay_stage[...].astype(BF16), preferred_element_type=F32)
        for g in range(GROUPS):
            spill_out[g] = spilled[g * SPILL : (g + 1) * SPILL].astype(BF16)
        send_all(spill_copy)
        spill_in[me] = spill_out[me]

        @pl.loop(early, batches)
        def _(batch):
            serve(batch)

    rows[me] = send_rows[me]
    receive_all(row_copy)
    if relayed:
        receive_all(spill_copy)
        for g in range(GROUPS):
            spill_stage[g * SPILL : (g + 1) * SPILL] = spill_in[g].astype(F32)

    def cols_copy(step, hop, target):
        source = agree_out.at[step] if hop == 0 else agree_out.at[2 + step]
        return pltpu.make_async_remote_copy(
            src_ref=source,
            dst_ref=agree_in.at[2 * step + hop],
            send_sem=cols_send.at[2 * step + hop],
            recv_sem=cols_recv.at[2 * step + hop],
            device_id={"cols": target},
            device_id_type=MESH,
        )

    lane_of = lax.broadcasted_iota(jnp.int32, (8, LANES), 1)
    wide = 2 * LANES // cap

    def landed(i):
        return jnp.concatenate([rows[i * wide + k] for k in range(wide)], axis=0)

    def weigh(i):
        both = jnp.concatenate([weights[2 * i], weights[2 * i + 1]], axis=1)
        return jnp.dot(both, landed(i), preferred_element_type=F32)

    for step in range(ITERS):
        summed = lax.fori_loop(
            0,
            main_tiles // 8,
            lambda i, acc: acc
            + ((weigh(4 * i) + weigh(4 * i + 1)) + (weigh(4 * i + 2) + weigh(4 * i + 3))),
            jnp.zeros((pairs, half), F32),
        )
        if relayed:
            spilled = spill_stage[...].astype(BF16)
            summed = summed + jnp.dot(weights[main_tiles], spilled, preferred_element_type=F32)
        partial = jnp.sum(summed * summed, axis=1, keepdims=True)
        packed = jnp.zeros((8, LANES), F32)
        for user in range(users):
            packed = jnp.where(lane_of == user, partial[user * 8 : user * 8 + 8], packed)
        if step + 1 < ITERS:
            parts = jnp.concatenate(split_two(summed), axis=0)

            def agree(tile, count, block):
                product = lax.dot_general(parts, block, NT, preferred_element_type=F32)
                product = product[:pairs] + product[pairs:]
                for k in range(count):
                    picked = users_of[tile + k]
                    own = jnp.zeros((8, LANES), F32)
                    for user in range(users):
                        piece = product[user * 8 : user * 8 + 8, k * LANES : (k + 1) * LANES]
                        own = jnp.where(picked == user, piece, own)
                    agree_out[step, tile + k] = own

            @pl.loop(0, main_tiles // 4)
            def _(i):
                for k in range(2):
                    agree(4 * i + 2 * k, 2, landed(2 * i + k))

            if relayed:
                agree(main_tiles, 1, spilled)
            agree_out[step, tiles] = packed
            cols_copy(step, 0, partner).start()
            cols_copy(step, 0, partner).wait_recv()
            agree_out[2 + step] = agree_out[step] + agree_in[2 * step]
            cols_copy(step, 1, cross).start()
            cols_copy(step, 1, cross).wait_recv()
            squares = agree_out[2 + step, tiles] + agree_in[2 * step + 1, tiles]
            scale = squash_scale(squares)
            scales = [jnp.broadcast_to(scale[:, user : user + 1], (8, LANES)) for user in range(users)]

            def next_weights(tile):
                picked = users_of[tile]
                factor = jnp.zeros((8, LANES), F32)
                for user in range(users):
                    factor = jnp.where(picked == user, scales[user], factor)
                total = agree_out[2 + step, tile] + agree_in[2 * step + 1, tile]
                value = logits[tile] + factor * total
                logits[tile] = value
                store_weights(tile, value)

            each_tile(next_weights)

        else:
            square_out[...] = packed
            copies = []
            for slot, target in enumerate((partner, cross, diagonal)):
                copies.append(
                    pltpu.make_async_remote_copy(
                        src_ref=square_out,
                        dst_ref=square_in.at[slot],
                        send_sem=sq_send.at[slot],
                        recv_sem=sq_recv.at[slot],
                        device_id={"cols": target},
                        device_id_type=MESH,
                    )
                )
            for copy in copies:
                copy.start()
            for copy in copies:
                copy.wait_recv()
            squares = (square_out[...] + square_in[0]) + (square_in[1] + square_in[2])
            scale = squash_scale(squares)
            for user in range(users):
                out_ref[user] = summed[user * 8 : user * 8 + 8] * scale[:, user : user + 1]
            for copy in copies:
                copy.wait_send()

    for part in range(CHUNKS):
        table_copy(part, cross, 0).wait_send()
        table_copy(part, partner, 1).wait_send()
        relay_copy(part).wait_send()

    @pl.loop(1, GROUPS)
    def _(step):
        request_copy(group_at(step), me).wait_send()
        row_copy(group_at(step), me).wait_send()
        if relayed:
            ask_copy(group_at(step), me).wait_send()
            hop_copy(group_at(step), me).wait_send()
            spill_copy(group_at(step), me).wait_send()

    for step in range(ITERS - 1):
        cols_copy(step, 0, partner).wait_send()
        cols_copy(step, 1, cross).wait_send()


def routed(cap, collective_id, item_ids, lengths, seed_rows, item_table, bilinear, seed_table):
    users, hist = item_ids.shape
    rows_dev, half = item_table.shape
    capsules = seed_table.shape[1]
    tiles = GROUPS * cap // LANES + (1 if cap < LANES else 0)
    vmem = pl.BlockSpec(memory_space=pltpu.VMEM)
    dma = pltpu.SemaphoreType.DMA
    return pl.pallas_call(
        functools.partial(kernel, cap),
        out_shape=[
            jax.ShapeDtypeStruct((users, capsules, half), F32),
            jax.ShapeDtypeStruct((8, LANES), jnp.int32),
        ],
        in_specs=[vmem, pl.BlockSpec(memory_space=pltpu.SMEM), vmem, vmem, vmem, vmem],
        out_specs=[vmem, vmem],
        scratch_shapes=[
            pltpu.VMEM((GROUPS, 1, LANES), jnp.int32),
            pltpu.VMEM((GROUPS, 1, LANES), jnp.int32),
            pltpu.VMEM((tiles, 8, LANES), jnp.int32),
            pltpu.VMEM((tiles, 8, LANES), jnp.int32),
            pltpu.VMEM((COLS, rows_dev, half), BF16),
            pltpu.VMEM((rows_dev, half), BF16),
            pltpu.VMEM((GROUPS, cap, half), BF16),
            pltpu.VMEM((GROUPS, cap, half), BF16),
            pltpu.VMEM((tiles, 8, LANES), F32),
            pltpu.VMEM((tiles, users * capsules, LANES), BF16),
            pltpu.VMEM((4, tiles + 1, 8, LANES), F32),
            pltpu.VMEM((4, tiles + 1, 8, LANES), F32),
            pltpu.VMEM((8, LANES), F32),
            pltpu.VMEM((3, 8, LANES), F32),
            pltpu.VMEM((GROUPS, 1, LANES), jnp.int32),
            pltpu.VMEM((GROUPS, 1, LANES), jnp.int32),
            pltpu.VMEM((GROUPS, HOP, half), BF16),
            pltpu.VMEM((GROUPS, HOP, half), BF16),
            pltpu.VMEM((GROUPS * HOP, half), F32),
            pltpu.VMEM((GROUPS, SPILL, half), BF16),
            pltpu.VMEM((GROUPS, SPILL, half), BF16),
            pltpu.VMEM((GROUPS * SPILL, half), F32),
            dma((GROUPS,)), dma((GROUPS,)),
            dma((2, CHUNKS)), dma((2, CHUNKS)), dma((CHUNKS,)), dma((CHUNKS,)),
            dma((GROUPS,)), dma((GROUPS,)),
            dma((4,)), dma((4,)), dma((3,)), dma((3,)),
            dma((GROUPS,)), dma((GROUPS,)), dma((GROUPS,)), dma((GROUPS,)),
            dma((GROUPS,)), dma((GROUPS,)),
        ],
        compiler_params=pltpu.CompilerParams(
            collective_id=collective_id, has_side_effects=True, vmem_limit_bytes=56 << 20
        ),
    )(item_ids, lengths, seed_rows, item_table, bilinear, seed_table)


def on_device(item_ids, lengths, seed_rows, item_table, bilinear, seed_table):
    maps = bilinear.reshape(COLS, -1, bilinear.shape[1])
    args = (item_ids, lengths, seed_rows, item_table, maps, seed_table)
    fast, fail = routed(64, 0, *args)
    return lax.cond(fail[0, 0] > 0, lambda: routed(LANES, 1, *args)[0], lambda: fast)


def solution(mesh):
    placed = (
        P("users", None),
        P("users"),
        P("users", None),
        P("users", "cols"),
        P(None, "cols"),
        P(),
    )
    return jax.shard_map(
        on_device, mesh=mesh, in_specs=placed, out_specs=P("users", None, "cols"), check_vma=False
    )
```

```python
import functools

import jax
import jax.numpy as jnp
from jax import lax
from jax.experimental import pallas as pl
from jax.experimental.pallas import tpu as pltpu
from jax.sharding import PartitionSpec as P

ITERS = 3
GROUPS = 64
COLS = 4
LANES = 128
BATCH = 8
CHUNKS = 4
HOP = 4
EARLY = 16
SPANS = ((0, 8), (8, 16), (16, 24), (24, 32))
SPILL = 2
MESH = pl.DeviceIdType.MESH
BF16 = jnp.bfloat16
F32 = jnp.float32
NT = (((1,), (1,)), ((), ()))


def squash_scale(squares):
    return squares / (1.0 + squares) / jnp.sqrt(squares + 1e-06)


def split_two(value):
    high = value.astype(BF16)
    low = (value - high.astype(F32)).astype(BF16)
    return high, low


def softmax_rows(logits):
    shifted = jnp.exp(logits - jnp.max(logits, axis=0, keepdims=True))
    return (shifted / jnp.sum(shifted, axis=0, keepdims=True)).astype(BF16)


def kernel(
    cap,
    ids_ref, len_ref, seed_ref, table_ref, map_ref, seed_table_ref,
    out_ref, fail_ref,
    req_out, req_in, users_of, seeds_of, gathered, mapped, send_rows, rows, send_early, rows_early,
    logits, weights, agree_out, agree_in, square_out, square_in,
    ask_out, ask_in, relay_rows_out, relay_rows_in, relay_stage, spill_out, spill_in, spill_stage,
    req_send, req_recv, tab_send, tab_recv, relay_send, relay_recv,
    row_send, row_recv, cols_send, cols_recv, sq_send, sq_recv,
    ask_send, ask_recv, hop_send, hop_recv, spill_send, spill_recv, early_send, early_recv,
):
    me = lax.axis_index("users")
    col = lax.axis_index("cols")
    users, hist = ids_ref.shape
    rows_dev = table_ref.shape[0]
    half = table_ref.shape[1]
    capsules = seed_table_ref.shape[0]
    pairs = users * capsules
    relayed = cap < LANES
    main_tiles = GROUPS * cap // LANES
    tiles = main_tiles + (1 if relayed else 0)
    per_tile = LANES // cap
    chunk = rows_dev // CHUNKS
    partner = col + 1 - 2 * lax.rem(col, 2)
    cross = lax.rem(col + 2, COLS)
    diagonal = lax.rem(partner + 2, COLS)

    def group_at(step):
        pair = lax.rem(me // 2 + step // 2, GROUPS // 2)
        return 2 * pair + lax.rem(me + step, 2)

    barrier = pltpu.get_barrier_semaphore()

    @pl.loop(1, GROUPS)
    def _(step):
        pl.semaphore_signal(barrier, inc=1, device_id={"users": group_at(step)}, device_id_type=MESH)

    for other in (partner, cross, diagonal):
        pl.semaphore_signal(barrier, inc=1, device_id={"cols": other}, device_id_type=MESH)

    position = lax.broadcasted_iota(jnp.int32, (1, hist), 1)
    owner_iota = lax.broadcasted_iota(jnp.int32, (GROUPS, hist), 0)
    tile_iota = lax.broadcasted_iota(jnp.int32, (tiles, hist), 0)
    rank_iota = lax.broadcasted_iota(jnp.int32, (LANES, hist), 0)
    upper = (
        lax.broadcasted_iota(jnp.int32, (hist, hist), 0)
        <= lax.broadcasted_iota(jnp.int32, (hist, hist), 1)
    ).astype(F32).astype(BF16)
    ones = jnp.ones((hist, hist), BF16)
    tri = jnp.concatenate([upper, ones], axis=0)
    before = jnp.zeros((GROUPS, hist), F32)
    before_first = jnp.zeros((GROUPS, hist), F32)
    owners, in_rows, ranks = [], [], []
    for user in range(users):
        ids = ids_ref[user : user + 1, :]
        owner = ids // rows_dev
        in_rows.append(ids - owner * rows_dev)
        owner = jnp.where(position < len_ref[user], owner, -1)
        owners.append(owner)
        onehot = jnp.where(owner_iota == owner, 1.0, 0.0)
        both = jnp.concatenate([onehot.astype(BF16), before.astype(BF16)], axis=1)
        counts = jnp.dot(both, tri, preferred_element_type=F32)
        before = before + onehot
        rank = jnp.sum(counts * onehot, axis=0, keepdims=True) - 1.0
        if relayed:
            first = in_rows[user] < rows_dev // 2
            onehot_first = jnp.where(first, onehot, 0.0)
            both = jnp.concatenate([onehot_first.astype(BF16), before_first.astype(BF16)], axis=1)
            counts = jnp.dot(both, tri, preferred_element_type=F32)
            before_first = before_first + onehot_first
            rank_first = jnp.sum(counts * onehot, axis=0, keepdims=True)
            kept = jnp.minimum(rank_first, float(EARLY))
            reserved = jnp.logical_and(first, rank_first <= float(EARLY))
            rank = jnp.where(reserved, rank_first - 1.0, EARLY + rank - kept)
            rank = jnp.where(owner >= 0, rank, -1.0)
        ranks.append(rank.astype(jnp.int32))
    if relayed:
        over = [jnp.where(rank >= cap, 1.0, 0.0) for rank in ranks]
        over_rows = jnp.concatenate(over, axis=0)
        over_before = [jnp.zeros((1, hist), F32)]
        for user in range(users):
            over_before.append(over_before[-1] + over[user])
        sums = jnp.concatenate(over_before[:users], axis=0)
        both = jnp.concatenate([over_rows.astype(BF16), sums.astype(BF16)], axis=1)
        queue = (jnp.dot(both, tri, preferred_element_type=F32) - 1.0).astype(jnp.int32)
        over_total = jnp.sum(over_before[users], axis=1, keepdims=True)
    requests = jnp.zeros((3 * GROUPS, LANES), F32)
    meta = jnp.zeros((2 * tiles, LANES), F32)
    for user in range(users):
        owner, row, rank = owners[user], in_rows[user], ranks[user]
        target, place = owner, rank
        tile = owner // per_tile
        spot = rank + (owner - tile * per_tile) * cap
        tile = jnp.where(owner >= 0, tile, -1)
        if relayed:
            line = queue[user : user + 1, :]
            turn = line // GROUPS
            spills = rank >= cap
            fits = turn < SPILL
            relay = lax.rem(line + me * 9, GROUPS)
            target = jnp.where(spills, jnp.where(fits, relay, -1), owner)
            place = jnp.where(spills, cap + turn, rank)
            tile = jnp.where(spills, jnp.where(fits, main_tiles, -1), tile)
            spot = jnp.where(spills, relay * SPILL + turn, spot)
        onehot = jnp.where(owner_iota == target, 1.0, 0.0)
        high = (row // 256).astype(F32) + 8.0
        low = (row - row // 256 * 256).astype(F32)
        left = jnp.concatenate(
            [(onehot * part).astype(BF16) for part in (high, low, owner.astype(F32))], axis=0
        )
        at_place = jnp.where(rank_iota == place, 1.0, 0.0).astype(BF16)
        requests = requests + lax.dot_general(left, at_place, NT, preferred_element_type=F32)
        onehot_tile = jnp.where(tile_iota == tile, 1.0, 0.0)
        seeds = seed_ref[user : user + 1, :].astype(F32)
        left = jnp.concatenate(
            [(onehot_tile * (user + 1.0)).astype(BF16), (onehot_tile * seeds).astype(BF16)], axis=0
        )
        at_spot = jnp.where(rank_iota == spot, 1.0, 0.0).astype(BF16)
        meta = meta + lax.dot_general(left, at_spot, NT, preferred_element_type=F32)
    asked = (requests[:GROUPS] - 8.0) * 256.0 + requests[GROUPS : 2 * GROUPS]
    lane_all = lax.broadcasted_iota(jnp.int32, (GROUPS, LANES), 1)
    if relayed:
        whole = asked + requests[2 * GROUPS :] * float(rows_dev)
        asked = jnp.where(lane_all < cap, asked, whole)
    asked = jnp.where(requests[:GROUPS] > 0.0, asked, -1.0)
    if relayed:
        too_many = jnp.where(over_total > float(SPILL * GROUPS), 1.0, 0.0)
        asked = jnp.where(lane_all == LANES - 1, too_many, asked)
    asked = asked.astype(jnp.int32)
    for owner in range(GROUPS):
        req_out[owner] = asked[owner : owner + 1, :]
    user_ids = meta[:tiles].astype(jnp.int32) - 1
    seed_ids = meta[tiles:].astype(jnp.int32)
    for tile in range(tiles):
        users_of[tile] = jnp.broadcast_to(user_ids[tile : tile + 1, :], (8, LANES))
        seeds_of[tile] = jnp.broadcast_to(seed_ids[tile : tile + 1, :], (8, LANES))

    pl.semaphore_wait(barrier, GROUPS - 1 + COLS - 1)

    def table_copy(part, target, slot):
        return pltpu.make_async_remote_copy(
            src_ref=table_ref.at[pl.ds(part * chunk, chunk)],
            dst_ref=gathered.at[col, pl.ds(part * chunk, chunk)],
            send_sem=tab_send.at[slot, part],
            recv_sem=tab_recv.at[slot, part],
            device_id={"cols": target},
            device_id_type=MESH,
        )

    def relay_copy(part):
        return pltpu.make_async_remote_copy(
            src_ref=gathered.at[cross, pl.ds(part * chunk, chunk)],
            dst_ref=gathered.at[cross, pl.ds(part * chunk, chunk)],
            send_sem=relay_send.at[part],
            recv_sem=relay_recv.at[part],
            device_id={"cols": partner},
            device_id_type=MESH,
        )

    def users_copy(source, landing_in, sends, recvs, target, landing):
        return pltpu.make_async_remote_copy(
            src_ref=source.at[target],
            dst_ref=landing_in.at[landing],
            send_sem=sends.at[target],
            recv_sem=recvs.at[landing],
            device_id={"users": target},
            device_id_type=MESH,
        )

    request_copy = functools.partial(users_copy, req_out, req_in, req_send, req_recv)
    row_copy = functools.partial(users_copy, send_rows, rows, row_send, row_recv)
    early_copy = functools.partial(users_copy, send_early, rows_early, early_send, early_recv)
    ask_copy = functools.partial(users_copy, ask_out, ask_in, ask_send, ask_recv)
    hop_copy = functools.partial(users_copy, relay_rows_out, relay_rows_in, hop_send, hop_recv)
    spill_copy = functools.partial(users_copy, spill_out, spill_in, spill_send, spill_recv)

    def send_all(copy):
        @pl.loop(1, GROUPS)
        def _(step):
            copy(group_at(step), me).start()

    def source_at(step):
        pair = lax.rem(me // 2 + GROUPS // 2 - step // 2, GROUPS // 2)
        return 2 * pair + lax.rem(me + step, 2)

    def receive_all(copy):
        @pl.loop(1, GROUPS)
        def _(step):
            copy(source_at(step), source_at(step)).wait_recv()

    send_all(request_copy)
    for part in range(CHUNKS):
        table_copy(part, cross, 0).start()
    for part in range(CHUNKS):
        table_copy(part, partner, 1).start()
    req_in[me] = req_out[me]

    seed_table = seed_table_ref[...]
    seed_high, seed_low = split_two(seed_table)
    seed_rest = (seed_table - seed_high.astype(F32) - seed_low.astype(F32)).astype(BF16)
    seed_count = seed_table.shape[1]
    seed_iota = lax.broadcasted_iota(jnp.int32, (seed_count, LANES), 0)

    def store_weights(tile, value):
        picked = users_of[tile]
        routed = softmax_rows(value).astype(F32)
        stacked = jnp.concatenate(
            [jnp.where(picked == user, routed, 0.0) for user in range(users)], axis=0
        )
        weights[tile] = stacked.astype(BF16)

    def each_tile(body):
        @pl.loop(0, main_tiles // 4)
        def _(i):
            for k in range(4):
                body(4 * i + k)

        if relayed:
            body(main_tiles)

    def first_weights(tile):
        chosen = jnp.where(seed_iota == seeds_of[tile][0:1, :], 1.0, 0.0).astype(BF16)
        start = jnp.zeros((capsules, LANES), F32)
        for part in (seed_rest, seed_low, seed_high):
            start = start + jnp.dot(part, chosen, preferred_element_type=F32)
        logits[tile] = start
        store_weights(tile, start)

    each_tile(first_weights)

    receive_all(request_copy)

    if relayed:
        tokens = GROUPS * SPILL
        token_lane = lax.broadcasted_iota(jnp.int32, (GROUPS, tokens), 1)
        token_row = lax.broadcasted_iota(jnp.int32, (GROUPS, tokens), 0)
        message = jnp.concatenate([req_in[g] for g in range(GROUPS)], axis=0)
        wanted = jnp.zeros((GROUPS, tokens), F32)
        for turn in range(SPILL):
            column = message[:, cap + turn : cap + turn + 1].astype(F32) + 1.0
            wanted = jnp.where(token_lane == token_row * SPILL + turn, column, wanted)
        token = jnp.sum(wanted, axis=0, keepdims=True).astype(jnp.int32) - 1
        owner = token // rows_dev
        row = token - owner * rows_dev
        owner = jnp.where(token >= 0, owner, -1)
        onehot = jnp.where(token_row == owner, 1.0, 0.0)
        counts = jnp.dot(onehot.astype(BF16), upper[:tokens, :tokens], preferred_element_type=F32)
        rank = (jnp.sum(counts * onehot, axis=0, keepdims=True) - 1.0).astype(jnp.int32)
        high = (row // 256).astype(F32) + 8.0
        low = (row - row // 256 * 256).astype(F32)
        left = jnp.concatenate([(onehot * high).astype(BF16), (onehot * low).astype(BF16)], axis=0)
        at_rank = jnp.where(rank_iota[:, :tokens] == rank, 1.0, 0.0).astype(BF16)
        hops = lax.dot_general(left, at_rank, NT, preferred_element_type=F32)
        asked = (hops[:GROUPS] - 8.0) * 256.0 + hops[GROUPS:]
        asked = jnp.where(hops[:GROUPS] > 0.0, asked, -1.0)
        flags = jnp.where(lane_all == LANES - 1, message.astype(F32), 0.0)
        flags = jnp.max(jnp.max(flags, axis=0, keepdims=True), axis=1, keepdims=True)
        deep = jnp.max(rank.astype(F32), axis=1, keepdims=True)
        flags = jnp.maximum(flags, jnp.where(deep >= float(HOP), 1.0, 0.0))
        asked = jnp.where(lane_all == LANES - 1, flags, asked).astype(jnp.int32)
        for target in range(GROUPS):
            ask_out[target] = asked[target : target + 1, :]
        landed_at = jnp.where(owner >= 0, owner * HOP + rank, -1)
        landed_at = jnp.broadcast_to(landed_at, (8, tokens)).astype(F32).T.astype(jnp.int32)[:, 0:1]
        send_all(ask_copy)
        ask_in[me] = ask_out[me]

    batches = GROUPS // BATCH
    stride = 2 * batches

    def step_of(batch, item):
        return 2 * batch + stride * (item // 2) + item % 2

    def serve(batch, low, high, shard, out, copy):
        wanted = jnp.concatenate(
            [req_in[group_at(step_of(batch, item))] for item in range(BATCH)], axis=0
        )
        columns = wanted.astype(F32).T.astype(jnp.int32)
        size = high - low
        lane_iota = lax.broadcasted_iota(jnp.int32, (size, shard), 1)
        onehot = jnp.concatenate(
            [
                jnp.where(lane_iota == columns[low:high, item : item + 1], 1.0, 0.0).astype(BF16)
                for item in range(BATCH)
            ],
            axis=0,
        )
        served = jnp.dot(onehot, mapped[:shard], preferred_element_type=F32).astype(BF16)
        for item in range(BATCH):
            out[group_at(step_of(batch, item))] = served[item * size : (item + 1) * size]
        for item in range(BATCH):
            if item:
                copy(group_at(step_of(batch, item)), me).start()
            else:

                @pl.when(batch > 0)
                def _():
                    copy(group_at(step_of(batch, 0)), me).start()

    def map_parts(parts):
        for part in parts:
            table_copy(part, cross, 0).wait_recv()
            relay_copy(part).start()
        for part in parts:
            table_copy(part, partner, 1).wait_recv()
            relay_copy(part).wait_recv()
            span = pl.ds(part * chunk, chunk)
            value = jnp.dot(table_ref[span], map_ref[col], preferred_element_type=F32)
            for source in (partner, cross, diagonal):
                value = value + jnp.dot(
                    gathered[source, span], map_ref[source], preferred_element_type=F32
                )
            mapped[span] = value.astype(BF16)

    start_late = EARLY if relayed else 0
    if relayed:
        map_parts(range(CHUNKS // 2))

        @pl.loop(0, batches)
        def _(batch):
            serve(batch, 0, EARLY, rows_dev // 2, send_early, early_copy)

        rows_early[me] = send_early[me]
        map_parts(range(CHUNKS // 2, CHUNKS))
    else:
        map_parts(range(CHUNKS))

    if relayed:
        receive_all(ask_copy)
        message = jnp.concatenate([ask_in[g] for g in range(GROUPS)], axis=0).astype(F32)
        flags = jnp.where(lane_all == LANES - 1, message, 0.0)
        flags = jnp.max(jnp.max(flags, axis=0, keepdims=True), axis=1, keepdims=True)
        fail_ref[0, 0] = jnp.max(flags).astype(jnp.int32)
        columns = message.T.astype(jnp.int32)
        hop_iota = lax.broadcasted_iota(jnp.int32, (HOP, rows_dev), 1)
        onehot = jnp.concatenate(
            [
                jnp.where(hop_iota == columns[:HOP, g : g + 1], 1.0, 0.0)
                for g in range(GROUPS)
            ],
            axis=0,
        ).astype(BF16)
        served = jnp.dot(onehot, mapped[...], preferred_element_type=F32)
        for g in range(GROUPS):
            relay_rows_out[g] = served[g * HOP : (g + 1) * HOP].astype(BF16)
        send_all(hop_copy)
        relay_rows_in[me] = relay_rows_out[me]
    else:
        fail_ref[0, 0] = 0

    def serve_late(batch):
        serve(batch, start_late, cap, rows_dev, send_rows, row_copy)

    early = batches // 2 if relayed else batches

    @pl.loop(0, early)
    def _(batch):
        serve_late(batch)

    if relayed:
        receive_all(hop_copy)
        for g in range(GROUPS):
            relay_stage[g * HOP : (g + 1) * HOP] = relay_rows_in[g].astype(F32)
        hop_lane = lax.broadcasted_iota(jnp.int32, (tokens, GROUPS * HOP), 1)
        onehot = jnp.where(hop_lane == landed_at, 1.0, 0.0).astype(BF16)
        spilled = jnp.dot(onehot, relay_stage[...].astype(BF16), preferred_element_type=F32)
        for g in range(GROUPS):
            spill_out[g] = spilled[g * SPILL : (g + 1) * SPILL].astype(BF16)
        send_all(spill_copy)
        spill_in[me] = spill_out[me]

        @pl.loop(early, batches)
        def _(batch):
            serve_late(batch)

    rows[me] = send_rows[me]
    pair_tiles = LANES // cap

    def pair_rows(pair):
        pieces = []
        for k in range(pair_tiles):
            if relayed:
                pieces.append(rows_early[pair * pair_tiles + k])
            pieces.append(rows[pair * pair_tiles + k])
        return jnp.concatenate(pieces, axis=0)

    def two_tiles(first, second):
        both = jnp.concatenate([weights[first], weights[second]], axis=1)
        block = jnp.concatenate([pair_rows(first), pair_rows(second)], axis=0)
        return jnp.dot(both, block, preferred_element_type=F32)

    def landed_batch(batch, total):
        for item in range(BATCH):
            source = source_at(step_of(batch, item))
            if relayed:
                early_copy(source, source).wait_recv()
            row_copy(source, source).wait_recv()
        tile = [source_at(step_of(batch, 2 * k)) // 2 for k in range(BATCH // 2)]
        return total + (two_tiles(tile[0], tile[1]) + two_tiles(tile[2], tile[3]))

    if relayed:
        for item in range(1, BATCH):
            source = source_at(step_of(0, item))
            early_copy(source, source).wait_recv()
            row_copy(source, source).wait_recv()
        tile = [source_at(step_of(0, 2 * k)) // 2 for k in range(BATCH // 2)]
        first_sum = two_tiles(tile[0], tile[1]) + two_tiles(tile[2], tile[3])
        first_sum = lax.fori_loop(1, batches, landed_batch, first_sum)
        receive_all(spill_copy)
        for g in range(GROUPS):
            spill_stage[g * SPILL : (g + 1) * SPILL] = spill_in[g].astype(F32)

    else:
        receive_all(row_copy)

    spans = [(low * main_tiles // 32, high * main_tiles // 32) for low, high in SPANS]
    blocks = [(1 + low if low else 0, 1 + high) for low, high in spans]
    blocks[-1] = (blocks[-1][0], 1 + tiles)

    def cols_copy(step, hop, span, target):
        low, high = blocks[span]
        piece = pl.ds(low, high - low)
        slot = (2 * step + hop) * len(blocks) + span
        return pltpu.make_async_remote_copy(
            src_ref=agree_out.at[2 * hop + step, piece],
            dst_ref=agree_in.at[2 * step + hop, piece],
            send_sem=cols_send.at[slot],
            recv_sem=cols_recv.at[slot],
            device_id={"cols": target},
            device_id_type=MESH,
        )

    lane_of = lax.broadcasted_iota(jnp.int32, (8, LANES), 1)

    def forward(step, span):
        low, high = blocks[span]
        piece = pl.ds(low, high - low)
        cols_copy(step, 0, span, partner).wait_recv()
        agree_out[2 + step, piece] = agree_out[step, piece] + agree_in[2 * step, piece]
        cols_copy(step, 1, span, cross).start()

    for step in range(ITERS):
        if step == 0 and relayed:
            summed = first_sum
        else:
            summed = lax.fori_loop(
                0,
                main_tiles // 8,
                lambda i, acc: acc
                + (
                    (two_tiles(8 * i, 8 * i + 1) + two_tiles(8 * i + 2, 8 * i + 3))
                    + (two_tiles(8 * i + 4, 8 * i + 5) + two_tiles(8 * i + 6, 8 * i + 7))
                ),
                jnp.zeros((pairs, half), F32),
            )
        if relayed:
            spilled = spill_stage[...].astype(BF16)
            summed = summed + jnp.dot(weights[main_tiles], spilled, preferred_element_type=F32)
        partial = jnp.sum(summed * summed, axis=1, keepdims=True)
        packed = jnp.zeros((8, LANES), F32)
        for user in range(users):
            packed = jnp.where(lane_of == user, partial[user * 8 : user * 8 + 8], packed)
        if step + 1 < ITERS:
            parts = jnp.concatenate(split_two(summed), axis=0)

            def agree(tile, count, block):
                product = lax.dot_general(parts, block, NT, preferred_element_type=F32)
                product = product[:pairs] + product[pairs:]
                for k in range(count):
                    picked = users_of[tile + k]
                    own = jnp.zeros((8, LANES), F32)
                    for user in range(users):
                        piece = product[user * 8 : user * 8 + 8, k * LANES : (k + 1) * LANES]
                        own = jnp.where(picked == user, piece, own)
                    agree_out[step, 1 + tile + k] = own

            agree_out[step, 0] = packed
            for span, (low, high) in enumerate(spans):

                @pl.loop(low // 4, high // 4)
                def _(i):
                    for k in (0, 2):
                        tile = 4 * i + k
                        block = jnp.concatenate([pair_rows(tile), pair_rows(tile + 1)], axis=0)
                        agree(tile, 2, block)

                if relayed and high == main_tiles:
                    agree(main_tiles, 1, spilled)
                cols_copy(step, 0, span, partner).start()
                if span > 0:
                    forward(step, span - 1)
            forward(step, len(spans) - 1)

            for span, (low, high) in enumerate(spans):
                cols_copy(step, 1, span, cross).wait_recv()
                if span == 0:
                    scale = squash_scale(agree_out[2 + step, 0] + agree_in[2 * step + 1, 0])
                    scales = [
                        jnp.broadcast_to(scale[:, user : user + 1], (8, LANES)) for user in range(users)
                    ]

                def next_weights(tile):
                    picked = users_of[tile]
                    factor = jnp.zeros((8, LANES), F32)
                    for user in range(users):
                        factor = jnp.where(picked == user, scales[user], factor)
                    total = agree_out[2 + step, 1 + tile] + agree_in[2 * step + 1, 1 + tile]
                    value = logits[tile] + factor * total
                    logits[tile] = value
                    store_weights(tile, value)

                @pl.loop(low // 4, high // 4)
                def _(i):
                    for k in range(4):
                        next_weights(4 * i + k)

                if relayed and high == main_tiles:
                    next_weights(main_tiles)

        else:
            square_out[...] = packed
            copies = []
            for slot, target in enumerate((partner, cross, diagonal)):
                copies.append(
                    pltpu.make_async_remote_copy(
                        src_ref=square_out,
                        dst_ref=square_in.at[slot],
                        send_sem=sq_send.at[slot],
                        recv_sem=sq_recv.at[slot],
                        device_id={"cols": target},
                        device_id_type=MESH,
                    )
                )
            for copy in copies:
                copy.start()
            for copy in copies:
                copy.wait_recv()
            squares = (square_out[...] + square_in[0]) + (square_in[1] + square_in[2])
            scale = squash_scale(squares)
            for user in range(users):
                out_ref[user] = summed[user * 8 : user * 8 + 8] * scale[:, user : user + 1]
            for copy in copies:
                copy.wait_send()

    for part in range(CHUNKS):
        table_copy(part, cross, 0).wait_send()
        table_copy(part, partner, 1).wait_send()
        relay_copy(part).wait_send()

    @pl.loop(1, GROUPS)
    def _(step):
        request_copy(group_at(step), me).wait_send()
        row_copy(group_at(step), me).wait_send()
        if relayed:
            ask_copy(group_at(step), me).wait_send()
            hop_copy(group_at(step), me).wait_send()
            spill_copy(group_at(step), me).wait_send()
            early_copy(group_at(step), me).wait_send()

    for step in range(ITERS - 1):
        for span in range(len(spans)):
            cols_copy(step, 0, span, partner).wait_send()
            cols_copy(step, 1, span, cross).wait_send()


def routed(cap, collective_id, item_ids, lengths, seed_rows, item_table, bilinear, seed_table):
    users, hist = item_ids.shape
    rows_dev, half = item_table.shape
    capsules = seed_table.shape[0]
    late = cap - EARLY if cap < LANES else cap
    tiles = GROUPS * cap // LANES + (1 if cap < LANES else 0)
    vmem = pl.BlockSpec(memory_space=pltpu.VMEM)
    dma = pltpu.SemaphoreType.DMA
    return pl.pallas_call(
        functools.partial(kernel, cap),
        out_shape=[
            jax.ShapeDtypeStruct((users, capsules, half), F32),
            jax.ShapeDtypeStruct((1, 1), jnp.int32),
        ],
        in_specs=[vmem, pl.BlockSpec(memory_space=pltpu.SMEM), vmem, vmem, vmem, vmem],
        out_specs=[vmem, pl.BlockSpec(memory_space=pltpu.SMEM)],
        scratch_shapes=[
            pltpu.VMEM((GROUPS, 1, LANES), jnp.int32),
            pltpu.VMEM((GROUPS, 1, LANES), jnp.int32),
            pltpu.VMEM((tiles, 8, LANES), jnp.int32),
            pltpu.VMEM((tiles, 8, LANES), jnp.int32),
            pltpu.VMEM((COLS, rows_dev, half), BF16),
            pltpu.VMEM((rows_dev, half), BF16),
            pltpu.VMEM((GROUPS, late, half), BF16),
            pltpu.VMEM((GROUPS, late, half), BF16),
            pltpu.VMEM((GROUPS, EARLY, half), BF16),
            pltpu.VMEM((GROUPS, EARLY, half), BF16),
            pltpu.VMEM((tiles, 8, LANES), F32),
            pltpu.VMEM((tiles, users * capsules, LANES), BF16),
            pltpu.VMEM((4, tiles + 1, 8, LANES), F32),
            pltpu.VMEM((4, tiles + 1, 8, LANES), F32),
            pltpu.VMEM((8, LANES), F32),
            pltpu.VMEM((3, 8, LANES), F32),
            pltpu.VMEM((GROUPS, 1, LANES), jnp.int32),
            pltpu.VMEM((GROUPS, 1, LANES), jnp.int32),
            pltpu.VMEM((GROUPS, HOP, half), BF16),
            pltpu.VMEM((GROUPS, HOP, half), BF16),
            pltpu.VMEM((GROUPS * HOP, half), F32),
            pltpu.VMEM((GROUPS, SPILL, half), BF16),
            pltpu.VMEM((GROUPS, SPILL, half), BF16),
            pltpu.VMEM((GROUPS * SPILL, half), F32),
            dma((GROUPS,)), dma((GROUPS,)),
            dma((2, CHUNKS)), dma((2, CHUNKS)), dma((CHUNKS,)), dma((CHUNKS,)),
            dma((GROUPS,)), dma((GROUPS,)),
            dma((4 * len(SPANS),)), dma((4 * len(SPANS),)), dma((3,)), dma((3,)),
            dma((GROUPS,)), dma((GROUPS,)), dma((GROUPS,)), dma((GROUPS,)),
            dma((GROUPS,)), dma((GROUPS,)), dma((GROUPS,)), dma((GROUPS,)),
        ],
        compiler_params=pltpu.CompilerParams(
            collective_id=collective_id, has_side_effects=True, vmem_limit_bytes=56 << 20
        ),
    )(item_ids, lengths, seed_rows, item_table, bilinear, seed_table)


def on_device(item_ids, lengths, seed_rows, item_table, bilinear, seed_table):
    maps = bilinear.reshape(COLS, -1, bilinear.shape[1])
    args = (item_ids, lengths, seed_rows, item_table, maps, seed_table.T)
    fast, fail = routed(64, 0, *args)
    return lax.cond(fail[0, 0] > 0, lambda: routed(LANES, 1, *args)[0], lambda: fast)


def solution(mesh):
    placed = (
        P("users", None),
        P("users"),
        P("users", None),
        P("users", "cols"),
        P(None, "cols"),
        P(),
    )
    return jax.shard_map(
        on_device, mesh=mesh, in_specs=placed, out_specs=P("users", None, "cols"), check_vma=False
    )
```

```python
import functools

import jax
import jax.numpy as jnp
from jax import lax
from jax.experimental import pallas as pl
from jax.experimental.pallas import tpu as pltpu
from jax.sharding import PartitionSpec as P

ITERS = 3
GROUPS = 64
COLS = 4
LANES = 128
BATCH = 8
CHUNKS = 4
HOP = 4
WIDE = 32
PHASES = ((1, 8), (2, 8), (3, 16))
SPANS = ((0, 8), (8, 16), (16, 24), (24, 32))
SPILL = 2
MESH = pl.DeviceIdType.MESH
BF16 = jnp.bfloat16
F32 = jnp.float32
NT = (((1,), (1,)), ((), ()))


def squash_scale(squares):
    return squares / (1.0 + squares) / jnp.sqrt(squares + 1e-06)


def split_two(value):
    high = value.astype(BF16)
    low = (value - high.astype(F32)).astype(BF16)
    return high, low


def softmax_rows(logits):
    shifted = jnp.exp(logits - jnp.max(logits, axis=0, keepdims=True))
    return (shifted / jnp.sum(shifted, axis=0, keepdims=True)).astype(BF16)


def kernel(
    cap,
    ids_ref, len_ref, seed_ref, table_ref, map_ref, seed_table_ref,
    out_ref, fail_ref,
    req_out, req_in, users_of, seeds_of, gathered, mapped, send_rows, rows,
    logits, weights, agree_out, agree_in, square_out, square_in,
    ask_out, ask_in, relay_rows_out, relay_rows_in, relay_stage, spill_out, spill_in, spill_stage,
    req_send, req_recv, tab_send, tab_recv, relay_send, relay_recv,
    row_send, row_recv, cols_send, cols_recv, sq_send, sq_recv,
    ask_send, ask_recv, hop_send, hop_recv, spill_send, spill_recv, early_send, early_recv, hop_onehot, *early_refs,
):
    me = lax.axis_index("users")
    col = lax.axis_index("cols")
    users, hist = ids_ref.shape
    rows_dev = table_ref.shape[0]
    half = table_ref.shape[1]
    capsules = seed_table_ref.shape[0]
    pairs = users * capsules
    relayed = cap < LANES
    main_tiles = GROUPS * cap // LANES
    tiles = main_tiles + (1 if relayed else 0)
    per_tile = LANES // cap
    chunk = rows_dev // CHUNKS
    partner = col + 1 - 2 * lax.rem(col, 2)
    cross = lax.rem(col + 2, COLS)
    diagonal = lax.rem(partner + 2, COLS)
    phases = PHASES if relayed else ()
    early_rows = sum(size for _, size in phases)
    early_out, early_in = early_refs[: len(phases)], early_refs[len(phases) : 2 * len(phases)]

    def group_at(step):
        pair = lax.rem(me // 2 + step // 2, GROUPS // 2)
        return 2 * pair + lax.rem(me + step, 2)

    barrier = pltpu.get_barrier_semaphore()

    @pl.loop(1, GROUPS)
    def _(step):
        pl.semaphore_signal(barrier, inc=1, device_id={"users": group_at(step)}, device_id_type=MESH)

    for other in (partner, cross, diagonal):
        pl.semaphore_signal(barrier, inc=1, device_id={"cols": other}, device_id_type=MESH)

    position = lax.broadcasted_iota(jnp.int32, (1, hist), 1)
    owner_iota = lax.broadcasted_iota(jnp.int32, (GROUPS, hist), 0)
    tile_iota = lax.broadcasted_iota(jnp.int32, (tiles, hist), 0)
    rank_iota = lax.broadcasted_iota(jnp.int32, (LANES, hist), 0)
    upper = (
        lax.broadcasted_iota(jnp.int32, (hist, hist), 0)
        <= lax.broadcasted_iota(jnp.int32, (hist, hist), 1)
    ).astype(F32).astype(BF16)
    ones = jnp.ones((hist, hist), BF16)
    tri = jnp.concatenate([upper, ones], axis=0)
    before = jnp.zeros((GROUPS, hist), F32)
    before_phase = [jnp.zeros((GROUPS, hist), F32) for _ in phases]
    owners, in_rows, ranks = [], [], []
    for user in range(users):
        ids = ids_ref[user : user + 1, :]
        owner = ids // rows_dev
        in_rows.append(ids - owner * rows_dev)
        owner = jnp.where(position < len_ref[user], owner, -1)
        owners.append(owner)
        onehot = jnp.where(owner_iota == owner, 1.0, 0.0)
        both = jnp.concatenate([onehot.astype(BF16), before.astype(BF16)], axis=1)
        counts = jnp.dot(both, tri, preferred_element_type=F32)
        before = before + onehot
        rank = jnp.sum(counts * onehot, axis=0, keepdims=True) - 1.0
        free = rank + float(early_rows)
        done, base = 0, 0
        for k, (parts, size) in enumerate(phases):
            low_row, high_row = done * chunk, parts * chunk
            inside = jnp.logical_and(in_rows[user] >= low_row, in_rows[user] < high_row)
            onehot_in = jnp.where(inside, onehot, 0.0)
            both = jnp.concatenate([onehot_in.astype(BF16), before_phase[k].astype(BF16)], axis=1)
            counts = jnp.dot(both, tri, preferred_element_type=F32)
            before_phase[k] = before_phase[k] + onehot_in
            rank_in = jnp.sum(counts * onehot, axis=0, keepdims=True)
            free = free - jnp.minimum(rank_in, float(size))
            reserved = jnp.logical_and(inside, rank_in <= float(size))
            rank = jnp.where(reserved, base + rank_in - 1.0, rank)
            taken = reserved if k == 0 else jnp.logical_or(taken, reserved)
            done, base = parts, base + size
        if phases:
            rank = jnp.where(taken, rank, free)
            rank = jnp.where(owner >= 0, rank, -1.0)
        ranks.append(rank.astype(jnp.int32))
    if relayed:
        over = [jnp.where(rank >= cap, 1.0, 0.0) for rank in ranks]
        over_rows = jnp.concatenate(over, axis=0)
        over_before = [jnp.zeros((1, hist), F32)]
        for user in range(users):
            over_before.append(over_before[-1] + over[user])
        sums = jnp.concatenate(over_before[:users], axis=0)
        both = jnp.concatenate([over_rows.astype(BF16), sums.astype(BF16)], axis=1)
        queue = (jnp.dot(both, tri, preferred_element_type=F32) - 1.0).astype(jnp.int32)
        over_total = jnp.sum(over_before[users], axis=1, keepdims=True)
    requests = jnp.zeros((3 * GROUPS, LANES), F32)
    meta = jnp.zeros((2 * tiles, LANES), F32)
    for user in range(users):
        owner, row, rank = owners[user], in_rows[user], ranks[user]
        target, place = owner, rank
        tile = owner // per_tile
        spot = rank + (owner - tile * per_tile) * cap
        tile = jnp.where(owner >= 0, tile, -1)
        if relayed:
            line = queue[user : user + 1, :]
            turn = line // GROUPS
            spills = rank >= cap
            fits = turn < SPILL
            relay = lax.rem(line + me * 9, GROUPS)
            target = jnp.where(spills, jnp.where(fits, relay, -1), owner)
            place = jnp.where(spills, cap + turn, rank)
            tile = jnp.where(spills, jnp.where(fits, main_tiles, -1), tile)
            spot = jnp.where(spills, relay * SPILL + turn, spot)
        onehot = jnp.where(owner_iota == target, 1.0, 0.0)
        high = (row // 256).astype(F32) + 8.0
        low = (row - row // 256 * 256).astype(F32)
        left = jnp.concatenate(
            [(onehot * part).astype(BF16) for part in (high, low, owner.astype(F32))], axis=0
        )
        at_place = jnp.where(rank_iota == place, 1.0, 0.0).astype(BF16)
        requests = requests + lax.dot_general(left, at_place, NT, preferred_element_type=F32)
        onehot_tile = jnp.where(tile_iota == tile, 1.0, 0.0)
        seeds = seed_ref[user : user + 1, :].astype(F32)
        left = jnp.concatenate(
            [(onehot_tile * (user + 1.0)).astype(BF16), (onehot_tile * seeds).astype(BF16)], axis=0
        )
        at_spot = jnp.where(rank_iota == spot, 1.0, 0.0).astype(BF16)
        meta = meta + lax.dot_general(left, at_spot, NT, preferred_element_type=F32)
    asked = (requests[:GROUPS] - 8.0) * 256.0 + requests[GROUPS : 2 * GROUPS]
    lane_all = lax.broadcasted_iota(jnp.int32, (GROUPS, LANES), 1)
    if relayed:
        whole = asked + requests[2 * GROUPS :] * float(rows_dev)
        asked = jnp.where(lane_all < cap, asked, whole)
    asked = jnp.where(requests[:GROUPS] > 0.0, asked, -1.0)
    if relayed:
        too_many = jnp.where(over_total > float(SPILL * GROUPS), 1.0, 0.0)
        asked = jnp.where(lane_all == LANES - 1, too_many, asked)
    asked = asked.astype(jnp.int32)
    for owner in range(GROUPS):
        req_out[owner] = asked[owner : owner + 1, :]
    user_ids = meta[:tiles].astype(jnp.int32) - 1
    seed_ids = meta[tiles:].astype(jnp.int32)
    for tile in range(tiles):
        users_of[tile] = jnp.broadcast_to(user_ids[tile : tile + 1, :], (8, LANES))
        seeds_of[tile] = jnp.broadcast_to(seed_ids[tile : tile + 1, :], (8, LANES))

    pl.semaphore_wait(barrier, GROUPS - 1 + COLS - 1)

    def table_copy(part, target, slot):
        return pltpu.make_async_remote_copy(
            src_ref=table_ref.at[pl.ds(part * chunk, chunk)],
            dst_ref=gathered.at[col, pl.ds(part * chunk, chunk)],
            send_sem=tab_send.at[0],
            recv_sem=tab_recv.at[slot, part],
            device_id={"cols": target},
            device_id_type=MESH,
        )

    def relay_copy(part):
        return pltpu.make_async_remote_copy(
            src_ref=gathered.at[cross, pl.ds(part * chunk, chunk)],
            dst_ref=gathered.at[cross, pl.ds(part * chunk, chunk)],
            send_sem=tab_send.at[0],
            recv_sem=relay_recv.at[part],
            device_id={"cols": partner},
            device_id_type=MESH,
        )

    def users_copy(source, landing_in, send_sem, recv_sem, target, landing):
        return pltpu.make_async_remote_copy(
            src_ref=source.at[target],
            dst_ref=landing_in.at[landing],
            send_sem=send_sem,
            recv_sem=recv_sem,
            device_id={"users": target},
            device_id_type=MESH,
        )

    def several(source, landing_in, send_sem, recv_sem, count):
        return pltpu.make_async_remote_copy(
            src_ref=source.at[pl.ds(0, count)],
            dst_ref=landing_in.at[pl.ds(0, count)],
            send_sem=send_sem,
            recv_sem=recv_sem,
            device_id={"users": group_at(1)},
            device_id_type=MESH,
        )

    request_all = (req_out, req_in, req_send.at[0], req_recv.at[0])
    ask_all = (ask_out, ask_in, ask_send.at[0], ask_recv.at[0])
    hop_all = (relay_rows_out, relay_rows_in, hop_send.at[0], hop_recv.at[0])
    spill_all = (spill_out, spill_in, spill_send.at[0], spill_recv.at[0])
    early_all = [
        (early_out[k], early_in[k], early_send.at[k], early_recv.at[k]) for k in range(len(phases))
    ]

    def row_all(batch):
        return (send_rows, rows, row_send.at[0], row_recv.at[batch])

    def send_all(kind):
        @pl.loop(1, GROUPS)
        def _(step):
            users_copy(*kind, group_at(step), me).start()

    def receive_all(kind):
        several(*kind, GROUPS - 1).wait_recv()

    def all_left(kind):
        several(*kind, GROUPS - 1).wait_send()

    def source_at(step):
        pair = lax.rem(me // 2 + GROUPS // 2 - step // 2, GROUPS // 2)
        return 2 * pair + lax.rem(me + step, 2)

    for part in range(CHUNKS):
        table_copy(part, cross, 0).start()
    for part in range(CHUNKS):
        table_copy(part, partner, 1).start()
    send_all(request_all)
    req_in[me] = req_out[me]

    seed_table = seed_table_ref[...]
    seed_high, seed_low = split_two(seed_table)
    seed_rest = (seed_table - seed_high.astype(F32) - seed_low.astype(F32)).astype(BF16)
    seed_count = seed_table.shape[1]
    seed_iota = lax.broadcasted_iota(jnp.int32, (seed_count, LANES), 0)

    def store_weights(tile, value):
        picked = users_of[tile]
        routed = softmax_rows(value).astype(F32)
        stacked = jnp.concatenate(
            [jnp.where(picked == user, routed, 0.0) for user in range(users)], axis=0
        )
        weights[tile] = stacked.astype(BF16)

    def each_tile(body):
        @pl.loop(0, main_tiles // 4)
        def _(i):
            for k in range(4):
                body(4 * i + k)

        if relayed:
            body(main_tiles)

    def first_weights(tile):
        chosen = jnp.where(seed_iota == seeds_of[tile][0:1, :], 1.0, 0.0).astype(BF16)
        start = jnp.zeros((capsules, LANES), F32)
        for part in (seed_rest, seed_low, seed_high):
            start = start + jnp.dot(part, chosen, preferred_element_type=F32)
        logits[tile] = start
        store_weights(tile, start)

    each_tile(first_weights)

    receive_all(request_all)

    if relayed:
        tokens = GROUPS * SPILL
        token_lane = lax.broadcasted_iota(jnp.int32, (GROUPS, tokens), 1)
        token_row = lax.broadcasted_iota(jnp.int32, (GROUPS, tokens), 0)
        message = jnp.concatenate([req_in[g] for g in range(GROUPS)], axis=0)
        wanted = jnp.zeros((GROUPS, tokens), F32)
        for turn in range(SPILL):
            column = message[:, cap + turn : cap + turn + 1].astype(F32) + 1.0
            wanted = jnp.where(token_lane == token_row * SPILL + turn, column, wanted)
        token = jnp.sum(wanted, axis=0, keepdims=True).astype(jnp.int32) - 1
        owner = token // rows_dev
        row = token - owner * rows_dev
        owner = jnp.where(token >= 0, owner, -1)
        onehot = jnp.where(token_row == owner, 1.0, 0.0)
        counts = jnp.dot(onehot.astype(BF16), upper[:tokens, :tokens], preferred_element_type=F32)
        rank = (jnp.sum(counts * onehot, axis=0, keepdims=True) - 1.0).astype(jnp.int32)
        high = (row // 256).astype(F32) + 8.0
        low = (row - row // 256 * 256).astype(F32)
        left = jnp.concatenate([(onehot * high).astype(BF16), (onehot * low).astype(BF16)], axis=0)
        at_rank = jnp.where(rank_iota[:, :tokens] == rank, 1.0, 0.0).astype(BF16)
        hops = lax.dot_general(left, at_rank, NT, preferred_element_type=F32)
        asked = (hops[:GROUPS] - 8.0) * 256.0 + hops[GROUPS:]
        asked = jnp.where(hops[:GROUPS] > 0.0, asked, -1.0)
        flags = jnp.where(lane_all == LANES - 1, message.astype(F32), 0.0)
        flags = jnp.max(jnp.max(flags, axis=0, keepdims=True), axis=1, keepdims=True)
        deep = jnp.max(rank.astype(F32), axis=1, keepdims=True)
        flags = jnp.maximum(flags, jnp.where(deep >= float(HOP), 1.0, 0.0))
        asked = jnp.where(lane_all == LANES - 1, flags, asked).astype(jnp.int32)
        for target in range(GROUPS):
            ask_out[target] = asked[target : target + 1, :]
        landed_at = jnp.where(owner >= 0, owner * HOP + rank, -1)
        landed_at = jnp.broadcast_to(landed_at, (8, tokens)).astype(F32).T.astype(jnp.int32)[:, 0:1]
        send_all(ask_all)
        ask_in[me] = ask_out[me]

    batches = GROUPS // BATCH

    def step_of(batch, item, items=BATCH):
        return 2 * batch + 2 * (GROUPS // items) * (item // 2) + item % 2

    def serve(batch, items, low, high, first_row, last_row, kind):
        wanted = jnp.concatenate(
            [req_in[group_at(step_of(batch, item, items))] for item in range(items)], axis=0
        )
        columns = wanted.astype(F32).T.astype(jnp.int32)
        size, shard = high - low, last_row - first_row
        lane_iota = lax.broadcasted_iota(jnp.int32, (size, shard), 1) + first_row
        onehot = jnp.concatenate(
            [
                jnp.where(lane_iota == columns[low:high, item : item + 1], 1.0, 0.0).astype(BF16)
                for item in range(items)
            ],
            axis=0,
        )
        served = jnp.dot(onehot, mapped[first_row:last_row], preferred_element_type=F32).astype(BF16)
        for item in range(items):
            kind[0][group_at(step_of(batch, item, items))] = served[item * size : (item + 1) * size]
        for item in range(items):
            if item:
                users_copy(*kind, group_at(step_of(batch, item, items)), me).start()
            else:

                @pl.when(batch > 0)
                def _():
                    users_copy(*kind, group_at(step_of(batch, 0)), me).start()

    def map_parts(parts):
        for part in parts:
            table_copy(part, cross, 0).wait_recv()
            relay_copy(part).start()
        for part in parts:
            table_copy(part, partner, 1).wait_recv()
            relay_copy(part).wait_recv()
            span = pl.ds(part * chunk, chunk)
            value = jnp.dot(table_ref[span], map_ref[col], preferred_element_type=F32)
            for source in (partner, cross, diagonal):
                value = value + jnp.dot(
                    gathered[source, span], map_ref[source], preferred_element_type=F32
                )
            mapped[span] = value.astype(BF16)

    done, base = 0, 0
    for k, (parts, size) in enumerate(phases):
        map_parts(range(done, parts))

        for batch in range(GROUPS // WIDE):
            serve(batch, WIDE, base, base + size, done * chunk, parts * chunk, early_all[k])


        early_in[k][me] = early_out[k][me]
        done, base = parts, base + size
    if relayed:
        receive_all(ask_all)
        message = jnp.concatenate([ask_in[g] for g in range(GROUPS)], axis=0).astype(F32)
        flags = jnp.where(lane_all == LANES - 1, message, 0.0)
        flags = jnp.max(jnp.max(flags, axis=0, keepdims=True), axis=1, keepdims=True)
        fail_ref[0, 0] = jnp.max(flags).astype(jnp.int32)
        columns = message.T.astype(jnp.int32)
        hop_iota = lax.broadcasted_iota(jnp.int32, (HOP, rows_dev), 1)
        hop_onehot[...] = jnp.concatenate(
            [
                jnp.where(hop_iota == columns[:HOP, g : g + 1], 1.0, 0.0)
                for g in range(GROUPS)
            ],
            axis=0,
        ).astype(BF16)
    map_parts(range(done, CHUNKS))

    if relayed:
        onehot = hop_onehot[...]
        served = jnp.dot(onehot, mapped[...], preferred_element_type=F32)
        for g in range(GROUPS):
            relay_rows_out[g] = served[g * HOP : (g + 1) * HOP].astype(BF16)
        send_all(hop_all)
        relay_rows_in[me] = relay_rows_out[me]
    else:
        fail_ref[0, 0] = 0

    def serve_late(batch):
        serve(batch, BATCH, early_rows, cap, 0, rows_dev, row_all(batch))

    early = batches // 2 if relayed else batches

    @pl.loop(0, early)
    def _(batch):
        serve_late(batch)

    if relayed:
        receive_all(hop_all)
        for g in range(GROUPS):
            relay_stage[g * HOP : (g + 1) * HOP] = relay_rows_in[g].astype(F32)
        hop_lane = lax.broadcasted_iota(jnp.int32, (tokens, GROUPS * HOP), 1)
        onehot = jnp.where(hop_lane == landed_at, 1.0, 0.0).astype(BF16)
        spilled = jnp.dot(onehot, relay_stage[...].astype(BF16), preferred_element_type=F32)
        for g in range(GROUPS):
            spill_out[g] = spilled[g * SPILL : (g + 1) * SPILL].astype(BF16)
        send_all(spill_all)
        spill_in[me] = spill_out[me]

        @pl.loop(early, batches)
        def _(batch):
            serve_late(batch)

    rows[me] = send_rows[me]
    pair_tiles = LANES // cap

    def pair_rows(pair):
        pieces = []
        for k in range(pair_tiles):
            for landing_in in early_in:
                pieces.append(landing_in[pair * pair_tiles + k])
            pieces.append(rows[pair * pair_tiles + k])
        return jnp.concatenate(pieces, axis=0)

    def two_tiles(first, second):
        both = jnp.concatenate([weights[first], weights[second]], axis=1)
        block = jnp.concatenate([pair_rows(first), pair_rows(second)], axis=0)
        return jnp.dot(both, block, preferred_element_type=F32)

    def landed_batch(batch, total, count=BATCH):
        several(*row_all(batch), count).wait_recv()
        tile = [source_at(step_of(batch, 2 * k)) // 2 for k in range(BATCH // 2)]
        return total + (two_tiles(tile[0], tile[1]) + two_tiles(tile[2], tile[3]))

    if relayed:
        for kind in early_all:
            receive_all(kind)
        first_sum = landed_batch(0, jnp.zeros((pairs, half), F32), BATCH - 1)
        first_sum = lax.fori_loop(1, batches, landed_batch, first_sum)
        receive_all(spill_all)
        for g in range(GROUPS):
            spill_stage[g * SPILL : (g + 1) * SPILL] = spill_in[g].astype(F32)

    else:
        several(*row_all(0), BATCH - 1).wait_recv()

        @pl.loop(1, batches)
        def _(batch):
            several(*row_all(batch), BATCH).wait_recv()

    spans = [(low * main_tiles // 32, high * main_tiles // 32) for low, high in SPANS]
    blocks = [(1 + low if low else 0, 1 + high) for low, high in spans]
    blocks[-1] = (blocks[-1][0], 1 + tiles)

    def cols_copy(step, hop, span, target):
        low, high = blocks[span]
        piece = pl.ds(low, high - low)
        slot = (2 * step + hop) * len(blocks) + span
        return pltpu.make_async_remote_copy(
            src_ref=agree_out.at[2 * hop + step, piece],
            dst_ref=agree_in.at[2 * step + hop, piece],
            send_sem=cols_send.at[0],
            recv_sem=cols_recv.at[slot],
            device_id={"cols": target},
            device_id_type=MESH,
        )

    lane_of = lax.broadcasted_iota(jnp.int32, (8, LANES), 1)

    def forward(step, span):
        low, high = blocks[span]
        piece = pl.ds(low, high - low)
        cols_copy(step, 0, span, partner).wait_recv()
        agree_out[2 + step, piece] = agree_out[step, piece] + agree_in[2 * step, piece]
        cols_copy(step, 1, span, cross).start()

    for step in range(ITERS):
        if step == 0 and relayed:
            summed = first_sum
        else:
            summed = lax.fori_loop(
                0,
                main_tiles // 8,
                lambda i, acc: acc
                + (
                    (two_tiles(8 * i, 8 * i + 1) + two_tiles(8 * i + 2, 8 * i + 3))
                    + (two_tiles(8 * i + 4, 8 * i + 5) + two_tiles(8 * i + 6, 8 * i + 7))
                ),
                jnp.zeros((pairs, half), F32),
            )
        if relayed:
            spilled = spill_stage[...].astype(BF16)
            summed = summed + jnp.dot(weights[main_tiles], spilled, preferred_element_type=F32)
        partial = jnp.sum(summed * summed, axis=1, keepdims=True)
        packed = jnp.zeros((8, LANES), F32)
        for user in range(users):
            packed = jnp.where(lane_of == user, partial[user * 8 : user * 8 + 8], packed)
        if step + 1 < ITERS:
            parts = jnp.concatenate(split_two(summed), axis=0)

            def agree(tile, count, block):
                product = lax.dot_general(parts, block, NT, preferred_element_type=F32)
                product = product[:pairs] + product[pairs:]
                for k in range(count):
                    picked = users_of[tile + k]
                    own = jnp.zeros((8, LANES), F32)
                    for user in range(users):
                        piece = product[user * 8 : user * 8 + 8, k * LANES : (k + 1) * LANES]
                        own = jnp.where(picked == user, piece, own)
                    agree_out[step, 1 + tile + k] = own

            agree_out[step, 0] = packed
            for span, (low, high) in enumerate(spans):

                @pl.loop(low // 4, high // 4)
                def _(i):
                    for k in (0, 2):
                        tile = 4 * i + k
                        block = jnp.concatenate([pair_rows(tile), pair_rows(tile + 1)], axis=0)
                        agree(tile, 2, block)

                if relayed and high == main_tiles:
                    agree(main_tiles, 1, spilled)
                cols_copy(step, 0, span, partner).start()
                if span > 0:
                    forward(step, span - 1)
            forward(step, len(spans) - 1)

            for span, (low, high) in enumerate(spans):
                cols_copy(step, 1, span, cross).wait_recv()
                if span == 0:
                    scale = squash_scale(agree_out[2 + step, 0] + agree_in[2 * step + 1, 0])
                    scales = [
                        jnp.broadcast_to(scale[:, user : user + 1], (8, LANES)) for user in range(users)
                    ]

                def next_weights(tile):
                    picked = users_of[tile]
                    factor = jnp.zeros((8, LANES), F32)
                    for user in range(users):
                        factor = jnp.where(picked == user, scales[user], factor)
                    total = agree_out[2 + step, 1 + tile] + agree_in[2 * step + 1, 1 + tile]
                    value = logits[tile] + factor * total
                    logits[tile] = value
                    store_weights(tile, value)

                @pl.loop(low // 4, high // 4)
                def _(i):
                    for k in range(4):
                        next_weights(4 * i + k)

                if relayed and high == main_tiles:
                    next_weights(main_tiles)

        else:
            square_out[...] = packed
            copies = []
            for slot, target in enumerate((partner, cross, diagonal)):
                copies.append(
                    pltpu.make_async_remote_copy(
                        src_ref=square_out,
                        dst_ref=square_in.at[slot],
                        send_sem=sq_send.at[slot],
                        recv_sem=sq_recv.at[slot],
                        device_id={"cols": target},
                        device_id_type=MESH,
                    )
                )
            for copy in copies:
                copy.start()
            for copy in copies:
                copy.wait_recv()
            squares = (square_out[...] + square_in[0]) + (square_in[1] + square_in[2])
            scale = squash_scale(squares)
            for user in range(users):
                out_ref[user] = summed[user * 8 : user * 8 + 8] * scale[:, user : user + 1]
            for copy in copies:
                copy.wait_send()

    def left(source, sem):
        pltpu.make_async_remote_copy(
            src_ref=source,
            dst_ref=source,
            send_sem=sem,
            recv_sem=tab_recv.at[0, 0],
            device_id={"cols": partner},
            device_id_type=MESH,
        ).wait_send()

    left(gathered.at[pl.ds(0, COLS - 1)], tab_send.at[0])
    left(agree_out, cols_send.at[0])
    all_left(request_all)
    all_left(row_all(0))
    if relayed:
        for kind in [ask_all, hop_all, spill_all] + early_all:
            all_left(kind)


def routed(cap, collective_id, item_ids, lengths, seed_rows, item_table, bilinear, seed_table):
    users, hist = item_ids.shape
    rows_dev, half = item_table.shape
    capsules = seed_table.shape[0]
    late = cap - sum(size for _, size in PHASES) if cap < LANES else cap
    phases = [size for _, size in PHASES]
    tiles = GROUPS * cap // LANES + (1 if cap < LANES else 0)
    vmem = pl.BlockSpec(memory_space=pltpu.VMEM)
    dma = pltpu.SemaphoreType.DMA
    return pl.pallas_call(
        functools.partial(kernel, cap),
        out_shape=[
            jax.ShapeDtypeStruct((users, capsules, half), F32),
            jax.ShapeDtypeStruct((1, 1), jnp.int32),
        ],
        in_specs=[vmem, pl.BlockSpec(memory_space=pltpu.SMEM), vmem, vmem, vmem, vmem],
        out_specs=[vmem, pl.BlockSpec(memory_space=pltpu.SMEM)],
        scratch_shapes=[
            pltpu.VMEM((GROUPS, 1, LANES), jnp.int32),
            pltpu.VMEM((GROUPS, 1, LANES), jnp.int32),
            pltpu.VMEM((tiles, 8, LANES), jnp.int32),
            pltpu.VMEM((tiles, 8, LANES), jnp.int32),
            pltpu.VMEM((COLS, rows_dev, half), BF16),
            pltpu.VMEM((rows_dev, half), BF16),
            pltpu.VMEM((GROUPS, late, half), BF16),
            pltpu.VMEM((GROUPS, late, half), BF16),
            pltpu.VMEM((tiles, 8, LANES), F32),
            pltpu.VMEM((tiles, users * capsules, LANES), BF16),
            pltpu.VMEM((4, tiles + 1, 8, LANES), F32),
            pltpu.VMEM((4, tiles + 1, 8, LANES), F32),
            pltpu.VMEM((8, LANES), F32),
            pltpu.VMEM((3, 8, LANES), F32),
            pltpu.VMEM((GROUPS, 1, LANES), jnp.int32),
            pltpu.VMEM((GROUPS, 1, LANES), jnp.int32),
            pltpu.VMEM((GROUPS, HOP, half), BF16),
            pltpu.VMEM((GROUPS, HOP, half), BF16),
            pltpu.VMEM((GROUPS * HOP, half), F32),
            pltpu.VMEM((GROUPS, SPILL, half), BF16),
            pltpu.VMEM((GROUPS, SPILL, half), BF16),
            pltpu.VMEM((GROUPS * SPILL, half), F32),
            dma((1,)), dma((1,)),
            dma((1,)), dma((2, CHUNKS)), dma((1,)), dma((CHUNKS,)),
            dma((1,)), dma((GROUPS // BATCH,)),
            dma((1,)), dma((4 * len(SPANS),)), dma((3,)), dma((3,)),
            dma((1,)), dma((1,)), dma((1,)), dma((1,)),
            dma((1,)), dma((1,)), dma((len(PHASES),)), dma((len(PHASES),)),
            pltpu.VMEM((GROUPS * HOP, rows_dev), BF16),
            *[pltpu.VMEM((GROUPS, size, half), BF16) for size in phases + phases],
        ],
        compiler_params=pltpu.CompilerParams(
            collective_id=collective_id, has_side_effects=True, vmem_limit_bytes=56 << 20
        ),
    )(item_ids, lengths, seed_rows, item_table, bilinear, seed_table)


def on_device(item_ids, lengths, seed_rows, item_table, bilinear, seed_table):
    maps = bilinear.reshape(COLS, -1, bilinear.shape[1])
    args = (item_ids, lengths, seed_rows, item_table, maps, seed_table.T)
    fast, fail = routed(64, 0, *args)
    return lax.cond(fail[0, 0] > 0, lambda: routed(LANES, 1, *args)[0], lambda: fast)


def solution(mesh):
    placed = (
        P("users", None),
        P("users"),
        P("users", None),
        P("users", "cols"),
        P(None, "cols"),
        P(),
    )
    return jax.shard_map(
        on_device, mesh=mesh, in_specs=placed, out_specs=P("users", None, "cols"), check_vma=False
    )
```

```python
import functools

import jax
import jax.numpy as jnp
from jax import lax
from jax.experimental import pallas as pl
from jax.experimental.pallas import tpu as pltpu
from jax.sharding import PartitionSpec as P

ITERS = 3
GROUPS = 64
COLS = 4
LANES = 128
BATCH = 8
CHUNKS = 4
HOP = 4
WIDE = 32
PHASES = ((1, 8), (2, 8), (3, 16))
SPANS = ((0, 8), (8, 16), (16, 24), (24, 32))
SPILL = 2
MESH = pl.DeviceIdType.MESH
BF16 = jnp.bfloat16
F32 = jnp.float32
NT = (((1,), (1,)), ((), ()))


def squash_scale(squares):
    return squares / (1.0 + squares) / jnp.sqrt(squares + 1e-06)


def split_two(value):
    high = value.astype(BF16)
    low = (value - high.astype(F32)).astype(BF16)
    return high, low


def softmax_rows(logits):
    shifted = jnp.exp(logits - jnp.max(logits, axis=0, keepdims=True))
    return (shifted / jnp.sum(shifted, axis=0, keepdims=True)).astype(BF16)


def kernel(
    cap,
    ids_ref, len_ref, seed_ref, table_ref, map_ref, seed_table_ref,
    out_ref, fail_ref,
    req_out, req_in, users_of, seeds_of, gathered, mapped, send_rows, rows,
    logits, weights, agree_out, agree_in, square_out, square_in,
    ask_out, ask_in, relay_rows_out, relay_rows_in, relay_stage, spill_out, spill_in, spill_stage,
    req_send, req_recv, tab_send, tab_recv, relay_send, relay_recv,
    row_send, row_recv, cols_send, cols_recv, sq_send, sq_recv,
    ask_send, ask_recv, hop_send, hop_recv, spill_send, spill_recv, early_send, early_recv, hop_onehot, *early_refs,
):
    me = lax.axis_index("users")
    col = lax.axis_index("cols")
    users, hist = ids_ref.shape
    rows_dev = table_ref.shape[0]
    half = table_ref.shape[1]
    capsules = seed_table_ref.shape[0]
    pairs = users * capsules
    relayed = cap < LANES
    main_tiles = GROUPS * cap // LANES
    tiles = main_tiles + (1 if relayed else 0)
    per_tile = LANES // cap
    chunk = rows_dev // CHUNKS
    partner = col + 1 - 2 * lax.rem(col, 2)
    cross = lax.rem(col + 2, COLS)
    diagonal = lax.rem(partner + 2, COLS)
    phases = PHASES if relayed else ()
    early_rows = sum(size for _, size in phases)
    early_out, early_in = early_refs[: len(phases)], early_refs[len(phases) : 2 * len(phases)]

    def group_at(step):
        pair = lax.rem(me // 2 + step // 2, GROUPS // 2)
        return 2 * pair + lax.rem(me + step, 2)

    barrier = pltpu.get_barrier_semaphore()

    @pl.loop(1, GROUPS)
    def _(step):
        pl.semaphore_signal(barrier, inc=1, device_id={"users": group_at(step)}, device_id_type=MESH)

    for other in (partner, cross, diagonal):
        pl.semaphore_signal(barrier, inc=1, device_id={"cols": other}, device_id_type=MESH)

    position = lax.broadcasted_iota(jnp.int32, (1, hist), 1)
    owner_iota = lax.broadcasted_iota(jnp.int32, (GROUPS, hist), 0)
    tile_iota = lax.broadcasted_iota(jnp.int32, (tiles, hist), 0)
    rank_iota = lax.broadcasted_iota(jnp.int32, (LANES, hist), 0)
    upper = (
        lax.broadcasted_iota(jnp.int32, (hist, hist), 0)
        <= lax.broadcasted_iota(jnp.int32, (hist, hist), 1)
    ).astype(F32).astype(BF16)
    ones = jnp.ones((hist, hist), BF16)
    tri = jnp.concatenate([upper, ones], axis=0)
    before = jnp.zeros((GROUPS, hist), F32)
    before_phase = [jnp.zeros((GROUPS, hist), F32) for _ in phases]
    owners, in_rows, ranks = [], [], []
    for user in range(users):
        ids = ids_ref[user : user + 1, :]
        owner = ids // rows_dev
        in_rows.append(ids - owner * rows_dev)
        owner = jnp.where(position < len_ref[user], owner, -1)
        owners.append(owner)
        onehot = jnp.where(owner_iota == owner, 1.0, 0.0)
        both = jnp.concatenate([onehot.astype(BF16), before.astype(BF16)], axis=1)
        counts = jnp.dot(both, tri, preferred_element_type=F32)
        before = before + onehot
        rank = jnp.sum(counts * onehot, axis=0, keepdims=True) - 1.0
        free = rank + float(early_rows)
        done, base = 0, 0
        for k, (parts, size) in enumerate(phases):
            low_row, high_row = done * chunk, parts * chunk
            inside = jnp.logical_and(in_rows[user] >= low_row, in_rows[user] < high_row)
            onehot_in = jnp.where(inside, onehot, 0.0)
            both = jnp.concatenate([onehot_in.astype(BF16), before_phase[k].astype(BF16)], axis=1)
            counts = jnp.dot(both, tri, preferred_element_type=F32)
            before_phase[k] = before_phase[k] + onehot_in
            rank_in = jnp.sum(counts * onehot, axis=0, keepdims=True)
            free = free - jnp.minimum(rank_in, float(size))
            reserved = jnp.logical_and(inside, rank_in <= float(size))
            rank = jnp.where(reserved, base + rank_in - 1.0, rank)
            taken = reserved if k == 0 else jnp.logical_or(taken, reserved)
            done, base = parts, base + size
        if phases:
            rank = jnp.where(taken, rank, free)
            rank = jnp.where(owner >= 0, rank, -1.0)
        ranks.append(rank.astype(jnp.int32))
    if relayed:
        over = [jnp.where(rank >= cap, 1.0, 0.0) for rank in ranks]
        over_rows = jnp.concatenate(over, axis=0)
        over_before = [jnp.zeros((1, hist), F32)]
        for user in range(users):
            over_before.append(over_before[-1] + over[user])
        sums = jnp.concatenate(over_before[:users], axis=0)
        both = jnp.concatenate([over_rows.astype(BF16), sums.astype(BF16)], axis=1)
        queue = (jnp.dot(both, tri, preferred_element_type=F32) - 1.0).astype(jnp.int32)
        over_total = jnp.sum(over_before[users], axis=1, keepdims=True)
    requests = jnp.zeros((3 * GROUPS, LANES), F32)
    meta = jnp.zeros((2 * tiles, LANES), F32)
    for user in range(users):
        owner, row, rank = owners[user], in_rows[user], ranks[user]
        target, place = owner, rank
        tile = owner // per_tile
        spot = rank + (owner - tile * per_tile) * cap
        tile = jnp.where(owner >= 0, tile, -1)
        if relayed:
            line = queue[user : user + 1, :]
            turn = line // GROUPS
            spills = rank >= cap
            fits = turn < SPILL
            relay = lax.rem(line + me * 9, GROUPS)
            target = jnp.where(spills, jnp.where(fits, relay, -1), owner)
            place = jnp.where(spills, cap + turn, rank)
            tile = jnp.where(spills, jnp.where(fits, main_tiles, -1), tile)
            spot = jnp.where(spills, relay * SPILL + turn, spot)
        onehot = jnp.where(owner_iota == target, 1.0, 0.0)
        high = (row // 256).astype(F32) + 8.0
        low = (row - row // 256 * 256).astype(F32)
        left = jnp.concatenate(
            [(onehot * part).astype(BF16) for part in (high, low, owner.astype(F32))], axis=0
        )
        at_place = jnp.where(rank_iota == place, 1.0, 0.0).astype(BF16)
        requests = requests + lax.dot_general(left, at_place, NT, preferred_element_type=F32)
        onehot_tile = jnp.where(tile_iota == tile, 1.0, 0.0)
        seeds = seed_ref[user : user + 1, :].astype(F32)
        left = jnp.concatenate(
            [(onehot_tile * (user + 1.0)).astype(BF16), (onehot_tile * seeds).astype(BF16)], axis=0
        )
        at_spot = jnp.where(rank_iota == spot, 1.0, 0.0).astype(BF16)
        meta = meta + lax.dot_general(left, at_spot, NT, preferred_element_type=F32)
    asked = (requests[:GROUPS] - 8.0) * 256.0 + requests[GROUPS : 2 * GROUPS]
    lane_all = lax.broadcasted_iota(jnp.int32, (GROUPS, LANES), 1)
    if relayed:
        whole = asked + requests[2 * GROUPS :] * float(rows_dev)
        asked = jnp.where(lane_all < cap, asked, whole)
    asked = jnp.where(requests[:GROUPS] > 0.0, asked, -1.0)
    if relayed:
        too_many = jnp.where(over_total > float(SPILL * GROUPS), 1.0, 0.0)
        asked = jnp.where(lane_all == LANES - 1, too_many, asked)
    asked = asked.astype(jnp.int32)
    for owner in range(GROUPS):
        req_out[owner] = asked[owner : owner + 1, :]
    user_ids = meta[:tiles].astype(jnp.int32) - 1
    seed_ids = meta[tiles:].astype(jnp.int32)
    for tile in range(tiles):
        users_of[tile] = jnp.broadcast_to(user_ids[tile : tile + 1, :], (8, LANES))
        seeds_of[tile] = jnp.broadcast_to(seed_ids[tile : tile + 1, :], (8, LANES))

    pl.semaphore_wait(barrier, GROUPS - 1 + COLS - 1)

    def table_copy(part, target, slot):
        return pltpu.make_async_remote_copy(
            src_ref=table_ref.at[pl.ds(part * chunk, chunk)],
            dst_ref=gathered.at[col, pl.ds(part * chunk, chunk)],
            send_sem=tab_send.at[0],
            recv_sem=tab_recv.at[slot, part],
            device_id={"cols": target},
            device_id_type=MESH,
        )

    def relay_copy(part):
        return pltpu.make_async_remote_copy(
            src_ref=gathered.at[cross, pl.ds(part * chunk, chunk)],
            dst_ref=gathered.at[cross, pl.ds(part * chunk, chunk)],
            send_sem=tab_send.at[0],
            recv_sem=relay_recv.at[part],
            device_id={"cols": partner},
            device_id_type=MESH,
        )

    def users_copy(source, landing_in, send_sem, recv_sem, target, landing):
        return pltpu.make_async_remote_copy(
            src_ref=source.at[target],
            dst_ref=landing_in.at[landing],
            send_sem=send_sem,
            recv_sem=recv_sem,
            device_id={"users": target},
            device_id_type=MESH,
        )

    def several(source, landing_in, send_sem, recv_sem, count):
        return pltpu.make_async_remote_copy(
            src_ref=source.at[pl.ds(0, count)],
            dst_ref=landing_in.at[pl.ds(0, count)],
            send_sem=send_sem,
            recv_sem=recv_sem,
            device_id={"users": group_at(1)},
            device_id_type=MESH,
        )

    request_all = (req_out, req_in, req_send.at[0], req_recv.at[0])
    ask_all = (ask_out, ask_in, ask_send.at[0], ask_recv.at[0])
    hop_all = (relay_rows_out, relay_rows_in, hop_send.at[0], hop_recv.at[0])
    spill_all = (spill_out, spill_in, spill_send.at[0], spill_recv.at[0])
    early_all = [
        (early_out[k], early_in[k], early_send.at[k], early_recv.at[k]) for k in range(len(phases))
    ]

    def row_all(batch):
        return (send_rows, rows, row_send.at[0], row_recv.at[batch])

    def send_all(kind):
        @pl.loop(1, GROUPS)
        def _(step):
            users_copy(*kind, group_at(step), me).start()

    def receive_all(kind):
        several(*kind, GROUPS - 1).wait_recv()

    def all_left(kind):
        several(*kind, GROUPS - 1).wait_send()

    def source_at(step):
        pair = lax.rem(me // 2 + GROUPS // 2 - step // 2, GROUPS // 2)
        return 2 * pair + lax.rem(me + step, 2)

    send_all(request_all)
    for part in range(CHUNKS):
        table_copy(part, cross, 0).start()
    for part in range(CHUNKS):
        table_copy(part, partner, 1).start()
    req_in[me] = req_out[me]

    seed_table = seed_table_ref[...]
    seed_high, seed_low = split_two(seed_table)
    seed_rest = (seed_table - seed_high.astype(F32) - seed_low.astype(F32)).astype(BF16)
    seed_count = seed_table.shape[1]
    seed_iota = lax.broadcasted_iota(jnp.int32, (seed_count, LANES), 0)

    def store_weights(tile, value):
        picked = users_of[tile]
        routed = softmax_rows(value).astype(F32)
        stacked = jnp.concatenate(
            [jnp.where(picked == user, routed, 0.0) for user in range(users)], axis=0
        )
        weights[tile] = stacked.astype(BF16)

    def each_tile(body):
        @pl.loop(0, main_tiles // 4)
        def _(i):
            for k in range(4):
                body(4 * i + k)

        if relayed:
            body(main_tiles)

    def first_weights(tile):
        chosen = jnp.where(seed_iota == seeds_of[tile][0:1, :], 1.0, 0.0).astype(BF16)
        start = jnp.zeros((capsules, LANES), F32)
        for part in (seed_rest, seed_low, seed_high):
            start = start + jnp.dot(part, chosen, preferred_element_type=F32)
        logits[tile] = start
        store_weights(tile, start)

    each_tile(first_weights)

    receive_all(request_all)

    if relayed:
        tokens = GROUPS * SPILL
        token_lane = lax.broadcasted_iota(jnp.int32, (GROUPS, tokens), 1)
        token_row = lax.broadcasted_iota(jnp.int32, (GROUPS, tokens), 0)
        message = jnp.concatenate([req_in[g] for g in range(GROUPS)], axis=0)
        wanted = jnp.zeros((GROUPS, tokens), F32)
        for turn in range(SPILL):
            column = message[:, cap + turn : cap + turn + 1].astype(F32) + 1.0
            wanted = jnp.where(token_lane == token_row * SPILL + turn, column, wanted)
        token = jnp.sum(wanted, axis=0, keepdims=True).astype(jnp.int32) - 1
        owner = token // rows_dev
        row = token - owner * rows_dev
        owner = jnp.where(token >= 0, owner, -1)
        onehot = jnp.where(token_row == owner, 1.0, 0.0)
        counts = jnp.dot(onehot.astype(BF16), upper[:tokens, :tokens], preferred_element_type=F32)
        rank = (jnp.sum(counts * onehot, axis=0, keepdims=True) - 1.0).astype(jnp.int32)
        high = (row // 256).astype(F32) + 8.0
        low = (row - row // 256 * 256).astype(F32)
        left = jnp.concatenate([(onehot * high).astype(BF16), (onehot * low).astype(BF16)], axis=0)
        at_rank = jnp.where(rank_iota[:, :tokens] == rank, 1.0, 0.0).astype(BF16)
        hops = lax.dot_general(left, at_rank, NT, preferred_element_type=F32)
        asked = (hops[:GROUPS] - 8.0) * 256.0 + hops[GROUPS:]
        asked = jnp.where(hops[:GROUPS] > 0.0, asked, -1.0)
        flags = jnp.where(lane_all == LANES - 1, message.astype(F32), 0.0)
        flags = jnp.max(jnp.max(flags, axis=0, keepdims=True), axis=1, keepdims=True)
        deep = jnp.max(rank.astype(F32), axis=1, keepdims=True)
        flags = jnp.maximum(flags, jnp.where(deep >= float(HOP), 1.0, 0.0))
        asked = jnp.where(lane_all == LANES - 1, flags, asked).astype(jnp.int32)
        for target in range(GROUPS):
            ask_out[target] = asked[target : target + 1, :]
        landed_at = jnp.where(owner >= 0, owner * HOP + rank, -1)
        landed_at = jnp.broadcast_to(landed_at, (8, tokens)).astype(F32).T.astype(jnp.int32)[:, 0:1]
        send_all(ask_all)
        ask_in[me] = ask_out[me]

    batches = GROUPS // BATCH

    def step_of(batch, item, items=BATCH):
        return 2 * batch + 2 * (GROUPS // items) * (item // 2) + item % 2

    def serve(batch, items, low, high, first_row, last_row, kind):
        wanted = jnp.concatenate(
            [req_in[group_at(step_of(batch, item, items))] for item in range(items)], axis=0
        )
        columns = wanted.astype(F32).T.astype(jnp.int32)
        size, shard = high - low, last_row - first_row
        lane_iota = lax.broadcasted_iota(jnp.int32, (size, shard), 1) + first_row
        onehot = jnp.concatenate(
            [
                jnp.where(lane_iota == columns[low:high, item : item + 1], 1.0, 0.0).astype(BF16)
                for item in range(items)
            ],
            axis=0,
        )
        served = jnp.dot(onehot, mapped[first_row:last_row], preferred_element_type=F32).astype(BF16)
        for item in range(items):
            kind[0][group_at(step_of(batch, item, items))] = served[item * size : (item + 1) * size]
        for item in range(items):
            if item:
                users_copy(*kind, group_at(step_of(batch, item, items)), me).start()
            else:

                @pl.when(batch > 0)
                def _():
                    users_copy(*kind, group_at(step_of(batch, 0)), me).start()

    def map_parts(parts):
        for part in parts:
            table_copy(part, cross, 0).wait_recv()
            relay_copy(part).start()
        for part in parts:
            table_copy(part, partner, 1).wait_recv()
            relay_copy(part).wait_recv()
            span = pl.ds(part * chunk, chunk)
            value = jnp.dot(table_ref[span], map_ref[col], preferred_element_type=F32)
            for source in (partner, cross, diagonal):
                value = value + jnp.dot(
                    gathered[source, span], map_ref[source], preferred_element_type=F32
                )
            mapped[span] = value.astype(BF16)

    done, base = 0, 0
    for k, (parts, size) in enumerate(phases):
        map_parts(range(done, parts))

        for batch in range(GROUPS // WIDE):
            serve(batch, WIDE, base, base + size, done * chunk, parts * chunk, early_all[k])


        early_in[k][me] = early_out[k][me]
        done, base = parts, base + size
    if relayed:
        receive_all(ask_all)
        message = jnp.concatenate([ask_in[g] for g in range(GROUPS)], axis=0).astype(F32)
        flags = jnp.where(lane_all == LANES - 1, message, 0.0)
        flags = jnp.max(jnp.max(flags, axis=0, keepdims=True), axis=1, keepdims=True)
        fail_ref[0, 0] = jnp.max(flags).astype(jnp.int32)
        columns = message.T.astype(jnp.int32)
        hop_iota = lax.broadcasted_iota(jnp.int32, (HOP, rows_dev), 1)
        hop_onehot[...] = jnp.concatenate(
            [
                jnp.where(hop_iota == columns[:HOP, g : g + 1], 1.0, 0.0)
                for g in range(GROUPS)
            ],
            axis=0,
        ).astype(BF16)
    map_parts(range(done, CHUNKS))

    if relayed:
        onehot = hop_onehot[...]
        served = jnp.dot(onehot, mapped[...], preferred_element_type=F32)
        for g in range(GROUPS):
            relay_rows_out[g] = served[g * HOP : (g + 1) * HOP].astype(BF16)
        send_all(hop_all)
        relay_rows_in[me] = relay_rows_out[me]
    else:
        fail_ref[0, 0] = 0

    def serve_late(batch):
        serve(batch, BATCH, early_rows, cap, 0, rows_dev, row_all(batch))

    early = batches // 2 if relayed else batches

    @pl.loop(0, early)
    def _(batch):
        serve_late(batch)

    if relayed:
        receive_all(hop_all)
        for g in range(GROUPS):
            relay_stage[g * HOP : (g + 1) * HOP] = relay_rows_in[g].astype(F32)
        hop_lane = lax.broadcasted_iota(jnp.int32, (tokens, GROUPS * HOP), 1)
        onehot = jnp.where(hop_lane == landed_at, 1.0, 0.0).astype(BF16)
        spilled = jnp.dot(onehot, relay_stage[...].astype(BF16), preferred_element_type=F32)
        for g in range(GROUPS):
            spill_out[g] = spilled[g * SPILL : (g + 1) * SPILL].astype(BF16)
        send_all(spill_all)
        spill_in[me] = spill_out[me]

        @pl.loop(early, batches)
        def _(batch):
            serve_late(batch)

    rows[me] = send_rows[me]
    pair_tiles = LANES // cap

    def pair_rows(pair):
        pieces = []
        for k in range(pair_tiles):
            for landing_in in early_in:
                pieces.append(landing_in[pair * pair_tiles + k])
            pieces.append(rows[pair * pair_tiles + k])
        return jnp.concatenate(pieces, axis=0)

    def two_tiles(first, second):
        both = jnp.concatenate([weights[first], weights[second]], axis=1)
        block = jnp.concatenate([pair_rows(first), pair_rows(second)], axis=0)
        return jnp.dot(both, block, preferred_element_type=F32)

    def landed_batch(batch, total, count=BATCH):
        several(*row_all(batch), count).wait_recv()
        tile = [source_at(step_of(batch, 2 * k)) // 2 for k in range(BATCH // 2)]
        return total + (two_tiles(tile[0], tile[1]) + two_tiles(tile[2], tile[3]))

    if relayed:
        for kind in early_all:
            receive_all(kind)
        first_sum = landed_batch(0, jnp.zeros((pairs, half), F32), BATCH - 1)
        first_sum = lax.fori_loop(1, batches, landed_batch, first_sum)
        receive_all(spill_all)
        for g in range(GROUPS):
            spill_stage[g * SPILL : (g + 1) * SPILL] = spill_in[g].astype(F32)

    else:
        several(*row_all(0), BATCH - 1).wait_recv()

        @pl.loop(1, batches)
        def _(batch):
            several(*row_all(batch), BATCH).wait_recv()

    spans = [(low * main_tiles // 32, high * main_tiles // 32) for low, high in SPANS]
    blocks = [(1 + low if low else 0, 1 + high) for low, high in spans]
    blocks[-1] = (blocks[-1][0], 1 + tiles)

    def cols_copy(step, hop, span, target):
        low, high = blocks[span]
        piece = pl.ds(low, high - low)
        slot = (2 * step + hop) * len(blocks) + span
        return pltpu.make_async_remote_copy(
            src_ref=agree_out.at[2 * hop + step, piece],
            dst_ref=agree_in.at[2 * step + hop, piece],
            send_sem=cols_send.at[0],
            recv_sem=cols_recv.at[slot],
            device_id={"cols": target},
            device_id_type=MESH,
        )

    lane_of = lax.broadcasted_iota(jnp.int32, (8, LANES), 1)

    def forward(step, span):
        low, high = blocks[span]
        piece = pl.ds(low, high - low)
        cols_copy(step, 0, span, partner).wait_recv()
        agree_out[2 + step, piece] = agree_out[step, piece] + agree_in[2 * step, piece]
        cols_copy(step, 1, span, cross).start()

    for step in range(ITERS):
        if step == 0 and relayed:
            summed = first_sum
        else:
            summed = lax.fori_loop(
                0,
                main_tiles // 8,
                lambda i, acc: acc
                + (
                    (two_tiles(8 * i, 8 * i + 1) + two_tiles(8 * i + 2, 8 * i + 3))
                    + (two_tiles(8 * i + 4, 8 * i + 5) + two_tiles(8 * i + 6, 8 * i + 7))
                ),
                jnp.zeros((pairs, half), F32),
            )
        if relayed:
            spilled = spill_stage[...].astype(BF16)
            summed = summed + jnp.dot(weights[main_tiles], spilled, preferred_element_type=F32)
        partial = jnp.sum(summed * summed, axis=1, keepdims=True)
        packed = jnp.zeros((8, LANES), F32)
        for user in range(users):
            packed = jnp.where(lane_of == user, partial[user * 8 : user * 8 + 8], packed)
        if step + 1 < ITERS:
            parts = jnp.concatenate(split_two(summed), axis=0)

            def agree(tile, count, block):
                product = lax.dot_general(parts, block, NT, preferred_element_type=F32)
                product = product[:pairs] + product[pairs:]
                for k in range(count):
                    picked = users_of[tile + k]
                    own = jnp.zeros((8, LANES), F32)
                    for user in range(users):
                        piece = product[user * 8 : user * 8 + 8, k * LANES : (k + 1) * LANES]
                        own = jnp.where(picked == user, piece, own)
                    agree_out[step, 1 + tile + k] = own

            agree_out[step, 0] = packed
            for span, (low, high) in enumerate(spans):

                @pl.loop(low // 4, high // 4)
                def _(i):
                    for k in (0, 2):
                        tile = 4 * i + k
                        block = jnp.concatenate([pair_rows(tile), pair_rows(tile + 1)], axis=0)
                        agree(tile, 2, block)

                if relayed and high == main_tiles:
                    agree(main_tiles, 1, spilled)
                cols_copy(step, 0, span, partner).start()
                if span > 0:
                    forward(step, span - 1)
            forward(step, len(spans) - 1)

            for span, (low, high) in enumerate(spans):
                cols_copy(step, 1, span, cross).wait_recv()
                if span == 0:
                    scale = squash_scale(agree_out[2 + step, 0] + agree_in[2 * step + 1, 0])
                    scales = [
                        jnp.broadcast_to(scale[:, user : user + 1], (8, LANES)) for user in range(users)
                    ]

                def next_weights(tile):
                    picked = users_of[tile]
                    factor = jnp.zeros((8, LANES), F32)
                    for user in range(users):
                        factor = jnp.where(picked == user, scales[user], factor)
                    total = agree_out[2 + step, 1 + tile] + agree_in[2 * step + 1, 1 + tile]
                    value = logits[tile] + factor * total
                    logits[tile] = value
                    store_weights(tile, value)

                @pl.loop(low // 4, high // 4)
                def _(i):
                    for k in range(4):
                        next_weights(4 * i + k)

                if relayed and high == main_tiles:
                    next_weights(main_tiles)

        else:
            square_out[...] = packed
            copies = []
            for slot, target in enumerate((partner, cross, diagonal)):
                copies.append(
                    pltpu.make_async_remote_copy(
                        src_ref=square_out,
                        dst_ref=square_in.at[slot],
                        send_sem=sq_send.at[slot],
                        recv_sem=sq_recv.at[slot],
                        device_id={"cols": target},
                        device_id_type=MESH,
                    )
                )
            for copy in copies:
                copy.start()
            for copy in copies:
                copy.wait_recv()
            squares = (square_out[...] + square_in[0]) + (square_in[1] + square_in[2])
            scale = squash_scale(squares)
            for user in range(users):
                out_ref[user] = summed[user * 8 : user * 8 + 8] * scale[:, user : user + 1]
            for copy in copies:
                copy.wait_send()

    def left(source, sem):
        pltpu.make_async_remote_copy(
            src_ref=source,
            dst_ref=source,
            send_sem=sem,
            recv_sem=tab_recv.at[0, 0],
            device_id={"cols": partner},
            device_id_type=MESH,
        ).wait_send()

    left(gathered.at[pl.ds(0, COLS - 1)], tab_send.at[0])
    left(agree_out, cols_send.at[0])
    all_left(request_all)
    all_left(row_all(0))
    if relayed:
        for kind in [ask_all, hop_all, spill_all] + early_all:
            all_left(kind)


def routed(cap, collective_id, item_ids, lengths, seed_rows, item_table, bilinear, seed_table):
    users, hist = item_ids.shape
    rows_dev, half = item_table.shape
    capsules = seed_table.shape[0]
    late = cap - sum(size for _, size in PHASES) if cap < LANES else cap
    phases = [size for _, size in PHASES]
    tiles = GROUPS * cap // LANES + (1 if cap < LANES else 0)
    vmem = pl.BlockSpec(memory_space=pltpu.VMEM)
    dma = pltpu.SemaphoreType.DMA
    return pl.pallas_call(
        functools.partial(kernel, cap),
        out_shape=[
            jax.ShapeDtypeStruct((users, capsules, half), F32),
            jax.ShapeDtypeStruct((1, 1), jnp.int32),
        ],
        in_specs=[vmem, pl.BlockSpec(memory_space=pltpu.SMEM), vmem, vmem, vmem, vmem],
        out_specs=[vmem, pl.BlockSpec(memory_space=pltpu.SMEM)],
        scratch_shapes=[
            pltpu.VMEM((GROUPS, 1, LANES), jnp.int32),
            pltpu.VMEM((GROUPS, 1, LANES), jnp.int32),
            pltpu.VMEM((tiles, 8, LANES), jnp.int32),
            pltpu.VMEM((tiles, 8, LANES), jnp.int32),
            pltpu.VMEM((COLS, rows_dev, half), BF16),
            pltpu.VMEM((rows_dev, half), BF16),
            pltpu.VMEM((GROUPS, late, half), BF16),
            pltpu.VMEM((GROUPS, late, half), BF16),
            pltpu.VMEM((tiles, 8, LANES), F32),
            pltpu.VMEM((tiles, users * capsules, LANES), BF16),
            pltpu.VMEM((4, tiles + 1, 8, LANES), F32),
            pltpu.VMEM((4, tiles + 1, 8, LANES), F32),
            pltpu.VMEM((8, LANES), F32),
            pltpu.VMEM((3, 8, LANES), F32),
            pltpu.VMEM((GROUPS, 1, LANES), jnp.int32),
            pltpu.VMEM((GROUPS, 1, LANES), jnp.int32),
            pltpu.VMEM((GROUPS, HOP, half), BF16),
            pltpu.VMEM((GROUPS, HOP, half), BF16),
            pltpu.VMEM((GROUPS * HOP, half), F32),
            pltpu.VMEM((GROUPS, SPILL, half), BF16),
            pltpu.VMEM((GROUPS, SPILL, half), BF16),
            pltpu.VMEM((GROUPS * SPILL, half), F32),
            dma((1,)), dma((1,)),
            dma((1,)), dma((2, CHUNKS)), dma((1,)), dma((CHUNKS,)),
            dma((1,)), dma((GROUPS // BATCH,)),
            dma((1,)), dma((4 * len(SPANS),)), dma((3,)), dma((3,)),
            dma((1,)), dma((1,)), dma((1,)), dma((1,)),
            dma((1,)), dma((1,)), dma((len(PHASES),)), dma((len(PHASES),)),
            pltpu.VMEM((GROUPS * HOP, rows_dev), BF16),
            *[pltpu.VMEM((GROUPS, size, half), BF16) for size in phases + phases],
        ],
        compiler_params=pltpu.CompilerParams(
            collective_id=collective_id, has_side_effects=True, vmem_limit_bytes=56 << 20
        ),
    )(item_ids, lengths, seed_rows, item_table, bilinear, seed_table)


def on_device(item_ids, lengths, seed_rows, item_table, bilinear, seed_table):
    maps = bilinear.reshape(COLS, -1, bilinear.shape[1])
    args = (item_ids, lengths, seed_rows, item_table, maps, seed_table.T)
    fast, fail = routed(64, 0, *args)
    return lax.cond(fail[0, 0] > 0, lambda: routed(LANES, 1, *args)[0], lambda: fast)


def solution(mesh):
    placed = (
        P("users", None),
        P("users"),
        P("users", None),
        P("users", "cols"),
        P(None, "cols"),
        P(),
    )
    return jax.shard_map(
        on_device, mesh=mesh, in_specs=placed, out_specs=P("users", None, "cols"), check_vma=False
    )
```

```python
import functools

import jax
import jax.numpy as jnp
from jax import lax
from jax.experimental import pallas as pl
from jax.experimental.pallas import tpu as pltpu
from jax.sharding import PartitionSpec as P

ITERS = 3
GROUPS = 64
COLS = 4
LANES = 128
BATCH = 8
CHUNKS = 4
HOP = 4
WIDE = 32
PHASES = ((1, 8), (2, 16), (3, 8))
SPANS = ((0, 8), (8, 16), (16, 24), (24, 32))
SPILL = 2
MESH = pl.DeviceIdType.MESH
BF16 = jnp.bfloat16
F32 = jnp.float32
NT = (((1,), (1,)), ((), ()))


def squash_scale(squares):
    return squares / (1.0 + squares) / jnp.sqrt(squares + 1e-06)


def split_two(value):
    high = value.astype(BF16)
    low = (value - high.astype(F32)).astype(BF16)
    return high, low


def softmax_rows(logits):
    shifted = jnp.exp(logits - jnp.max(logits, axis=0, keepdims=True))
    return (shifted / jnp.sum(shifted, axis=0, keepdims=True)).astype(BF16)


def kernel(
    cap,
    ids_ref, len_ref, seed_ref, table_ref, map_ref, seed_table_ref,
    out_ref, fail_ref,
    req_out, req_in, users_of, seeds_of, gathered, mapped, send_rows, rows,
    logits, weights, agree_out, agree_in, square_out, square_in,
    ask_out, ask_in, relay_rows_out, relay_rows_in, relay_stage, spill_out, spill_in, spill_stage,
    req_send, req_recv, tab_send, tab_recv, relay_send, relay_recv,
    row_send, row_recv, cols_send, cols_recv, sq_send, sq_recv,
    ask_send, ask_recv, hop_send, hop_recv, spill_send, spill_recv, early_send, early_recv, hop_onehot, *early_refs,
):
    me = lax.axis_index("users")
    col = lax.axis_index("cols")
    users, hist = ids_ref.shape
    rows_dev = table_ref.shape[0]
    half = table_ref.shape[1]
    capsules = seed_table_ref.shape[0]
    pairs = users * capsules
    relayed = cap < LANES
    main_tiles = GROUPS * cap // LANES
    tiles = main_tiles + (1 if relayed else 0)
    per_tile = LANES // cap
    chunk = rows_dev // CHUNKS
    partner = col + 1 - 2 * lax.rem(col, 2)
    cross = lax.rem(col + 2, COLS)
    diagonal = lax.rem(partner + 2, COLS)
    phases = PHASES if relayed else ()
    early_rows = sum(size for _, size in phases)
    early_out, early_in = early_refs[: len(phases)], early_refs[len(phases) : 2 * len(phases)]

    def group_at(step):
        pair = lax.rem(me // 2 + step // 2, GROUPS // 2)
        return 2 * pair + lax.rem(me + step, 2)

    barrier = pltpu.get_barrier_semaphore()

    @pl.loop(1, GROUPS)
    def _(step):
        pl.semaphore_signal(barrier, inc=1, device_id={"users": group_at(step)}, device_id_type=MESH)

    for other in (partner, cross, diagonal):
        pl.semaphore_signal(barrier, inc=1, device_id={"cols": other}, device_id_type=MESH)

    position = lax.broadcasted_iota(jnp.int32, (1, hist), 1)
    owner_iota = lax.broadcasted_iota(jnp.int32, (GROUPS, hist), 0)
    tile_iota = lax.broadcasted_iota(jnp.int32, (tiles, hist), 0)
    rank_iota = lax.broadcasted_iota(jnp.int32, (LANES, hist), 0)
    upper = (
        lax.broadcasted_iota(jnp.int32, (hist, hist), 0)
        <= lax.broadcasted_iota(jnp.int32, (hist, hist), 1)
    ).astype(F32).astype(BF16)
    ones = jnp.ones((hist, hist), BF16)
    tri = jnp.concatenate([upper, ones], axis=0)
    before = jnp.zeros((GROUPS, hist), F32)
    before_phase = [jnp.zeros((GROUPS, hist), F32) for _ in phases]
    owners, in_rows, ranks = [], [], []
    for user in range(users):
        ids = ids_ref[user : user + 1, :]
        owner = ids // rows_dev
        in_rows.append(ids - owner * rows_dev)
        owner = jnp.where(position < len_ref[user], owner, -1)
        owners.append(owner)
        onehot = jnp.where(owner_iota == owner, 1.0, 0.0)
        both = jnp.concatenate([onehot.astype(BF16), before.astype(BF16)], axis=1)
        counts = jnp.dot(both, tri, preferred_element_type=F32)
        before = before + onehot
        rank = jnp.sum(counts * onehot, axis=0, keepdims=True) - 1.0
        free = rank + float(early_rows)
        done, base = 0, 0
        for k, (parts, size) in enumerate(phases):
            low_row, high_row = done * chunk, parts * chunk
            inside = jnp.logical_and(in_rows[user] >= low_row, in_rows[user] < high_row)
            onehot_in = jnp.where(inside, onehot, 0.0)
            both = jnp.concatenate([onehot_in.astype(BF16), before_phase[k].astype(BF16)], axis=1)
            counts = jnp.dot(both, tri, preferred_element_type=F32)
            before_phase[k] = before_phase[k] + onehot_in
            rank_in = jnp.sum(counts * onehot, axis=0, keepdims=True)
            free = free - jnp.minimum(rank_in, float(size))
            reserved = jnp.logical_and(inside, rank_in <= float(size))
            rank = jnp.where(reserved, base + rank_in - 1.0, rank)
            taken = reserved if k == 0 else jnp.logical_or(taken, reserved)
            done, base = parts, base + size
        if phases:
            rank = jnp.where(taken, rank, free)
            rank = jnp.where(owner >= 0, rank, -1.0)
        ranks.append(rank.astype(jnp.int32))
    if relayed:
        over = [jnp.where(rank >= cap, 1.0, 0.0) for rank in ranks]
        over_rows = jnp.concatenate(over, axis=0)
        over_before = [jnp.zeros((1, hist), F32)]
        for user in range(users):
            over_before.append(over_before[-1] + over[user])
        sums = jnp.concatenate(over_before[:users], axis=0)
        both = jnp.concatenate([over_rows.astype(BF16), sums.astype(BF16)], axis=1)
        queue = (jnp.dot(both, tri, preferred_element_type=F32) - 1.0).astype(jnp.int32)
        over_total = jnp.sum(over_before[users], axis=1, keepdims=True)
    requests = jnp.zeros((3 * GROUPS, LANES), F32)
    meta = jnp.zeros((2 * tiles, LANES), F32)
    for user in range(users):
        owner, row, rank = owners[user], in_rows[user], ranks[user]
        target, place = owner, rank
        tile = owner // per_tile
        spot = rank + (owner - tile * per_tile) * cap
        tile = jnp.where(owner >= 0, tile, -1)
        if relayed:
            line = queue[user : user + 1, :]
            turn = line // GROUPS
            spills = rank >= cap
            fits = turn < SPILL
            relay = lax.rem(line + me * 9, GROUPS)
            target = jnp.where(spills, jnp.where(fits, relay, -1), owner)
            place = jnp.where(spills, cap + turn, rank)
            tile = jnp.where(spills, jnp.where(fits, main_tiles, -1), tile)
            spot = jnp.where(spills, relay * SPILL + turn, spot)
        onehot = jnp.where(owner_iota == target, 1.0, 0.0)
        high = (row // 256).astype(F32) + 8.0
        low = (row - row // 256 * 256).astype(F32)
        left = jnp.concatenate(
            [(onehot * part).astype(BF16) for part in (high, low, owner.astype(F32))], axis=0
        )
        at_place = jnp.where(rank_iota == place, 1.0, 0.0).astype(BF16)
        requests = requests + lax.dot_general(left, at_place, NT, preferred_element_type=F32)
        onehot_tile = jnp.where(tile_iota == tile, 1.0, 0.0)
        seeds = seed_ref[user : user + 1, :].astype(F32)
        left = jnp.concatenate(
            [(onehot_tile * (user + 1.0)).astype(BF16), (onehot_tile * seeds).astype(BF16)], axis=0
        )
        at_spot = jnp.where(rank_iota == spot, 1.0, 0.0).astype(BF16)
        meta = meta + lax.dot_general(left, at_spot, NT, preferred_element_type=F32)
    asked = (requests[:GROUPS] - 8.0) * 256.0 + requests[GROUPS : 2 * GROUPS]
    lane_all = lax.broadcasted_iota(jnp.int32, (GROUPS, LANES), 1)
    if relayed:
        whole = asked + requests[2 * GROUPS :] * float(rows_dev)
        asked = jnp.where(lane_all < cap, asked, whole)
    asked = jnp.where(requests[:GROUPS] > 0.0, asked, -1.0)
    if relayed:
        too_many = jnp.where(over_total > float(SPILL * GROUPS), 1.0, 0.0)
        asked = jnp.where(lane_all == LANES - 1, too_many, asked)
    asked = asked.astype(jnp.int32)
    for owner in range(GROUPS):
        req_out[owner] = asked[owner : owner + 1, :]
    user_ids = meta[:tiles].astype(jnp.int32) - 1
    seed_ids = meta[tiles:].astype(jnp.int32)
    for tile in range(tiles):
        users_of[tile] = jnp.broadcast_to(user_ids[tile : tile + 1, :], (8, LANES))
        seeds_of[tile] = jnp.broadcast_to(seed_ids[tile : tile + 1, :], (8, LANES))

    pl.semaphore_wait(barrier, GROUPS - 1 + COLS - 1)

    def table_copy(part, target, slot):
        return pltpu.make_async_remote_copy(
            src_ref=table_ref.at[pl.ds(part * chunk, chunk)],
            dst_ref=gathered.at[col, pl.ds(part * chunk, chunk)],
            send_sem=tab_send.at[0],
            recv_sem=tab_recv.at[slot, part],
            device_id={"cols": target},
            device_id_type=MESH,
        )

    def relay_copy(part):
        return pltpu.make_async_remote_copy(
            src_ref=gathered.at[cross, pl.ds(part * chunk, chunk)],
            dst_ref=gathered.at[cross, pl.ds(part * chunk, chunk)],
            send_sem=tab_send.at[0],
            recv_sem=relay_recv.at[part],
            device_id={"cols": partner},
            device_id_type=MESH,
        )

    def users_copy(source, landing_in, send_sem, recv_sem, target, landing):
        return pltpu.make_async_remote_copy(
            src_ref=source.at[target],
            dst_ref=landing_in.at[landing],
            send_sem=send_sem,
            recv_sem=recv_sem,
            device_id={"users": target},
            device_id_type=MESH,
        )

    def several(source, landing_in, send_sem, recv_sem, count):
        return pltpu.make_async_remote_copy(
            src_ref=source.at[pl.ds(0, count)],
            dst_ref=landing_in.at[pl.ds(0, count)],
            send_sem=send_sem,
            recv_sem=recv_sem,
            device_id={"users": group_at(1)},
            device_id_type=MESH,
        )

    request_all = (req_out, req_in, req_send.at[0], req_recv.at[0])
    ask_all = (ask_out, ask_in, ask_send.at[0], ask_recv.at[0])
    hop_all = (relay_rows_out, relay_rows_in, hop_send.at[0], hop_recv.at[0])
    spill_all = (spill_out, spill_in, spill_send.at[0], spill_recv.at[0])
    early_all = [
        (early_out[k], early_in[k], early_send.at[k], early_recv.at[k]) for k in range(len(phases))
    ]

    def row_all(batch):
        return (send_rows, rows, row_send.at[0], row_recv.at[batch])

    def send_all(kind):
        @pl.loop(1, GROUPS)
        def _(step):
            users_copy(*kind, group_at(step), me).start()

    def receive_all(kind):
        several(*kind, GROUPS - 1).wait_recv()

    def all_left(kind):
        several(*kind, GROUPS - 1).wait_send()

    def source_at(step):
        pair = lax.rem(me // 2 + GROUPS // 2 - step // 2, GROUPS // 2)
        return 2 * pair + lax.rem(me + step, 2)

    send_all(request_all)
    for part in range(CHUNKS):
        table_copy(part, cross, 0).start()
    for part in range(CHUNKS):
        table_copy(part, partner, 1).start()
    req_in[me] = req_out[me]

    seed_table = seed_table_ref[...]
    seed_high, seed_low = split_two(seed_table)
    seed_rest = (seed_table - seed_high.astype(F32) - seed_low.astype(F32)).astype(BF16)
    seed_count = seed_table.shape[1]
    seed_iota = lax.broadcasted_iota(jnp.int32, (seed_count, LANES), 0)

    def store_weights(tile, value):
        picked = users_of[tile]
        routed = softmax_rows(value).astype(F32)
        stacked = jnp.concatenate(
            [jnp.where(picked == user, routed, 0.0) for user in range(users)], axis=0
        )
        weights[tile] = stacked.astype(BF16)

    def each_tile(body):
        @pl.loop(0, main_tiles // 4)
        def _(i):
            for k in range(4):
                body(4 * i + k)

        if relayed:
            body(main_tiles)

    def first_weights(tile):
        chosen = jnp.where(seed_iota == seeds_of[tile][0:1, :], 1.0, 0.0).astype(BF16)
        start = jnp.zeros((capsules, LANES), F32)
        for part in (seed_rest, seed_low, seed_high):
            start = start + jnp.dot(part, chosen, preferred_element_type=F32)
        logits[tile] = start
        store_weights(tile, start)

    each_tile(first_weights)

    receive_all(request_all)

    if relayed:
        tokens = GROUPS * SPILL
        token_lane = lax.broadcasted_iota(jnp.int32, (GROUPS, tokens), 1)
        token_row = lax.broadcasted_iota(jnp.int32, (GROUPS, tokens), 0)
        message = jnp.concatenate([req_in[g] for g in range(GROUPS)], axis=0)
        wanted = jnp.zeros((GROUPS, tokens), F32)
        for turn in range(SPILL):
            column = message[:, cap + turn : cap + turn + 1].astype(F32) + 1.0
            wanted = jnp.where(token_lane == token_row * SPILL + turn, column, wanted)
        token = jnp.sum(wanted, axis=0, keepdims=True).astype(jnp.int32) - 1
        owner = token // rows_dev
        row = token - owner * rows_dev
        owner = jnp.where(token >= 0, owner, -1)
        onehot = jnp.where(token_row == owner, 1.0, 0.0)
        counts = jnp.dot(onehot.astype(BF16), upper[:tokens, :tokens], preferred_element_type=F32)
        rank = (jnp.sum(counts * onehot, axis=0, keepdims=True) - 1.0).astype(jnp.int32)
        high = (row // 256).astype(F32) + 8.0
        low = (row - row // 256 * 256).astype(F32)
        left = jnp.concatenate([(onehot * high).astype(BF16), (onehot * low).astype(BF16)], axis=0)
        at_rank = jnp.where(rank_iota[:, :tokens] == rank, 1.0, 0.0).astype(BF16)
        hops = lax.dot_general(left, at_rank, NT, preferred_element_type=F32)
        asked = (hops[:GROUPS] - 8.0) * 256.0 + hops[GROUPS:]
        asked = jnp.where(hops[:GROUPS] > 0.0, asked, -1.0)
        flags = jnp.where(lane_all == LANES - 1, message.astype(F32), 0.0)
        flags = jnp.max(jnp.max(flags, axis=0, keepdims=True), axis=1, keepdims=True)
        deep = jnp.max(rank.astype(F32), axis=1, keepdims=True)
        flags = jnp.maximum(flags, jnp.where(deep >= float(HOP), 1.0, 0.0))
        asked = jnp.where(lane_all == LANES - 1, flags, asked).astype(jnp.int32)
        for target in range(GROUPS):
            ask_out[target] = asked[target : target + 1, :]
        landed_at = jnp.where(owner >= 0, owner * HOP + rank, -1)
        landed_at = jnp.broadcast_to(landed_at, (8, tokens)).astype(F32).T.astype(jnp.int32)[:, 0:1]
        send_all(ask_all)
        ask_in[me] = ask_out[me]

    batches = GROUPS // BATCH

    def step_of(batch, item, items=BATCH):
        return 2 * batch + 2 * (GROUPS // items) * (item // 2) + item % 2

    def serve(batch, items, low, high, first_row, last_row, kind):
        wanted = jnp.concatenate(
            [req_in[group_at(step_of(batch, item, items))] for item in range(items)], axis=0
        )
        columns = wanted.astype(F32).T.astype(jnp.int32)
        size, shard = high - low, last_row - first_row
        lane_iota = lax.broadcasted_iota(jnp.int32, (size, shard), 1) + first_row
        onehot = jnp.concatenate(
            [
                jnp.where(lane_iota == columns[low:high, item : item + 1], 1.0, 0.0).astype(BF16)
                for item in range(items)
            ],
            axis=0,
        )
        served = jnp.dot(onehot, mapped[first_row:last_row], preferred_element_type=F32).astype(BF16)
        for item in range(items):
            kind[0][group_at(step_of(batch, item, items))] = served[item * size : (item + 1) * size]
        for item in range(items):
            if item:
                users_copy(*kind, group_at(step_of(batch, item, items)), me).start()
            else:

                @pl.when(batch > 0)
                def _():
                    users_copy(*kind, group_at(step_of(batch, 0)), me).start()

    def map_parts(parts):
        for part in parts:
            table_copy(part, cross, 0).wait_recv()
            relay_copy(part).start()
        for part in parts:
            table_copy(part, partner, 1).wait_recv()
            relay_copy(part).wait_recv()
            span = pl.ds(part * chunk, chunk)
            value = jnp.dot(table_ref[span], map_ref[col], preferred_element_type=F32)
            for source in (partner, cross, diagonal):
                value = value + jnp.dot(
                    gathered[source, span], map_ref[source], preferred_element_type=F32
                )
            mapped[span] = value.astype(BF16)

    done, base = 0, 0
    for k, (parts, size) in enumerate(phases):
        map_parts(range(done, parts))

        for batch in range(GROUPS // WIDE):
            serve(batch, WIDE, base, base + size, done * chunk, parts * chunk, early_all[k])


        early_in[k][me] = early_out[k][me]
        done, base = parts, base + size
    if relayed:
        receive_all(ask_all)
        message = jnp.concatenate([ask_in[g] for g in range(GROUPS)], axis=0).astype(F32)
        flags = jnp.where(lane_all == LANES - 1, message, 0.0)
        flags = jnp.max(jnp.max(flags, axis=0, keepdims=True), axis=1, keepdims=True)
        fail_ref[0, 0] = jnp.max(flags).astype(jnp.int32)
        columns = message.T.astype(jnp.int32)
        hop_iota = lax.broadcasted_iota(jnp.int32, (HOP, rows_dev), 1)
        hop_onehot[...] = jnp.concatenate(
            [
                jnp.where(hop_iota == columns[:HOP, g : g + 1], 1.0, 0.0)
                for g in range(GROUPS)
            ],
            axis=0,
        ).astype(BF16)
    map_parts(range(done, CHUNKS))

    if relayed:
        onehot = hop_onehot[...]
        served = jnp.dot(onehot, mapped[...], preferred_element_type=F32)
        for g in range(GROUPS):
            relay_rows_out[g] = served[g * HOP : (g + 1) * HOP].astype(BF16)
        send_all(hop_all)
        relay_rows_in[me] = relay_rows_out[me]
    else:
        fail_ref[0, 0] = 0

    def serve_late(batch):
        serve(batch, BATCH, early_rows, cap, 0, rows_dev, row_all(batch))

    early = batches // 2 if relayed else batches

    @pl.loop(0, early)
    def _(batch):
        serve_late(batch)

    if relayed:
        receive_all(hop_all)
        for g in range(GROUPS):
            relay_stage[g * HOP : (g + 1) * HOP] = relay_rows_in[g].astype(F32)
        hop_lane = lax.broadcasted_iota(jnp.int32, (tokens, GROUPS * HOP), 1)
        onehot = jnp.where(hop_lane == landed_at, 1.0, 0.0).astype(BF16)
        spilled = jnp.dot(onehot, relay_stage[...].astype(BF16), preferred_element_type=F32)
        for g in range(GROUPS):
            spill_out[g] = spilled[g * SPILL : (g + 1) * SPILL].astype(BF16)
        send_all(spill_all)
        spill_in[me] = spill_out[me]

        @pl.loop(early, batches)
        def _(batch):
            serve_late(batch)

    rows[me] = send_rows[me]
    pair_tiles = LANES // cap

    def pair_rows(pair):
        pieces = []
        for k in range(pair_tiles):
            for landing_in in early_in:
                pieces.append(landing_in[pair * pair_tiles + k])
            pieces.append(rows[pair * pair_tiles + k])
        return jnp.concatenate(pieces, axis=0)

    def two_tiles(first, second):
        both = jnp.concatenate([weights[first], weights[second]], axis=1)
        block = jnp.concatenate([pair_rows(first), pair_rows(second)], axis=0)
        return jnp.dot(both, block, preferred_element_type=F32)

    def landed_batch(batch, total, count=BATCH):
        several(*row_all(batch), count).wait_recv()
        tile = [source_at(step_of(batch, 2 * k)) // 2 for k in range(BATCH // 2)]
        return total + (two_tiles(tile[0], tile[1]) + two_tiles(tile[2], tile[3]))

    if relayed:
        for kind in early_all:
            receive_all(kind)
        first_sum = landed_batch(0, jnp.zeros((pairs, half), F32), BATCH - 1)
        first_sum = lax.fori_loop(1, batches, landed_batch, first_sum)
        receive_all(spill_all)
        for g in range(GROUPS):
            spill_stage[g * SPILL : (g + 1) * SPILL] = spill_in[g].astype(F32)

    else:
        several(*row_all(0), BATCH - 1).wait_recv()

        @pl.loop(1, batches)
        def _(batch):
            several(*row_all(batch), BATCH).wait_recv()

    spans = [(low * main_tiles // 32, high * main_tiles // 32) for low, high in SPANS]
    blocks = [(1 + low if low else 0, 1 + high) for low, high in spans]
    blocks[-1] = (blocks[-1][0], 1 + tiles)

    def cols_copy(step, hop, span, target):
        low, high = blocks[span]
        piece = pl.ds(low, high - low)
        slot = (2 * step + hop) * len(blocks) + span
        return pltpu.make_async_remote_copy(
            src_ref=agree_out.at[2 * hop + step, piece],
            dst_ref=agree_in.at[2 * step + hop, piece],
            send_sem=cols_send.at[0],
            recv_sem=cols_recv.at[slot],
            device_id={"cols": target},
            device_id_type=MESH,
        )

    lane_of = lax.broadcasted_iota(jnp.int32, (8, LANES), 1)

    def forward(step, span):
        low, high = blocks[span]
        piece = pl.ds(low, high - low)
        cols_copy(step, 0, span, partner).wait_recv()
        agree_out[2 + step, piece] = agree_out[step, piece] + agree_in[2 * step, piece]
        cols_copy(step, 1, span, cross).start()

    for step in range(ITERS):
        if step == 0 and relayed:
            summed = first_sum
        else:
            summed = lax.fori_loop(
                0,
                main_tiles // 8,
                lambda i, acc: acc
                + (
                    (two_tiles(8 * i, 8 * i + 1) + two_tiles(8 * i + 2, 8 * i + 3))
                    + (two_tiles(8 * i + 4, 8 * i + 5) + two_tiles(8 * i + 6, 8 * i + 7))
                ),
                jnp.zeros((pairs, half), F32),
            )
        if relayed:
            spilled = spill_stage[...].astype(BF16)
            summed = summed + jnp.dot(weights[main_tiles], spilled, preferred_element_type=F32)
        partial = jnp.sum(summed * summed, axis=1, keepdims=True)
        packed = jnp.zeros((8, LANES), F32)
        for user in range(users):
            packed = jnp.where(lane_of == user, partial[user * 8 : user * 8 + 8], packed)
        if step + 1 < ITERS:
            parts = jnp.concatenate(split_two(summed), axis=0)

            def agree(tile, count, block):
                product = lax.dot_general(parts, block, NT, preferred_element_type=F32)
                product = product[:pairs] + product[pairs:]
                for k in range(count):
                    picked = users_of[tile + k]
                    own = jnp.zeros((8, LANES), F32)
                    for user in range(users):
                        piece = product[user * 8 : user * 8 + 8, k * LANES : (k + 1) * LANES]
                        own = jnp.where(picked == user, piece, own)
                    agree_out[step, 1 + tile + k] = own

            agree_out[step, 0] = packed
            for span, (low, high) in enumerate(spans):

                @pl.loop(low // 4, high // 4)
                def _(i):
                    for k in (0, 2):
                        tile = 4 * i + k
                        block = jnp.concatenate([pair_rows(tile), pair_rows(tile + 1)], axis=0)
                        agree(tile, 2, block)

                if relayed and high == main_tiles:
                    agree(main_tiles, 1, spilled)
                cols_copy(step, 0, span, partner).start()
                if span > 0:
                    forward(step, span - 1)
            forward(step, len(spans) - 1)

            for span, (low, high) in enumerate(spans):
                cols_copy(step, 1, span, cross).wait_recv()
                if span == 0:
                    scale = squash_scale(agree_out[2 + step, 0] + agree_in[2 * step + 1, 0])
                    scales = [
                        jnp.broadcast_to(scale[:, user : user + 1], (8, LANES)) for user in range(users)
                    ]

                def next_weights(tile):
                    picked = users_of[tile]
                    factor = jnp.zeros((8, LANES), F32)
                    for user in range(users):
                        factor = jnp.where(picked == user, scales[user], factor)
                    total = agree_out[2 + step, 1 + tile] + agree_in[2 * step + 1, 1 + tile]
                    value = logits[tile] + factor * total
                    logits[tile] = value
                    store_weights(tile, value)

                @pl.loop(low // 4, high // 4)
                def _(i):
                    for k in range(4):
                        next_weights(4 * i + k)

                if relayed and high == main_tiles:
                    next_weights(main_tiles)

        else:
            square_out[...] = packed
            copies = []
            for slot, target in enumerate((partner, cross, diagonal)):
                copies.append(
                    pltpu.make_async_remote_copy(
                        src_ref=square_out,
                        dst_ref=square_in.at[slot],
                        send_sem=sq_send.at[slot],
                        recv_sem=sq_recv.at[slot],
                        device_id={"cols": target},
                        device_id_type=MESH,
                    )
                )
            for copy in copies:
                copy.start()
            for copy in copies:
                copy.wait_recv()
            squares = (square_out[...] + square_in[0]) + (square_in[1] + square_in[2])
            scale = squash_scale(squares)
            for user in range(users):
                out_ref[user] = summed[user * 8 : user * 8 + 8] * scale[:, user : user + 1]
            for copy in copies:
                copy.wait_send()

    def left(source, sem):
        pltpu.make_async_remote_copy(
            src_ref=source,
            dst_ref=source,
            send_sem=sem,
            recv_sem=tab_recv.at[0, 0],
            device_id={"cols": partner},
            device_id_type=MESH,
        ).wait_send()

    left(gathered.at[pl.ds(0, COLS - 1)], tab_send.at[0])
    left(agree_out, cols_send.at[0])
    all_left(request_all)
    all_left(row_all(0))
    if relayed:
        for kind in [ask_all, hop_all, spill_all] + early_all:
            all_left(kind)


def routed(cap, collective_id, item_ids, lengths, seed_rows, item_table, bilinear, seed_table):
    users, hist = item_ids.shape
    rows_dev, half = item_table.shape
    capsules = seed_table.shape[0]
    late = cap - sum(size for _, size in PHASES) if cap < LANES else cap
    phases = [size for _, size in PHASES]
    tiles = GROUPS * cap // LANES + (1 if cap < LANES else 0)
    vmem = pl.BlockSpec(memory_space=pltpu.VMEM)
    dma = pltpu.SemaphoreType.DMA
    return pl.pallas_call(
        functools.partial(kernel, cap),
        out_shape=[
            jax.ShapeDtypeStruct((users, capsules, half), F32),
            jax.ShapeDtypeStruct((1, 1), jnp.int32),
        ],
        in_specs=[vmem, pl.BlockSpec(memory_space=pltpu.SMEM), vmem, vmem, vmem, vmem],
        out_specs=[vmem, pl.BlockSpec(memory_space=pltpu.SMEM)],
        scratch_shapes=[
            pltpu.VMEM((GROUPS, 1, LANES), jnp.int32),
            pltpu.VMEM((GROUPS, 1, LANES), jnp.int32),
            pltpu.VMEM((tiles, 8, LANES), jnp.int32),
            pltpu.VMEM((tiles, 8, LANES), jnp.int32),
            pltpu.VMEM((COLS, rows_dev, half), BF16),
            pltpu.VMEM((rows_dev, half), BF16),
            pltpu.VMEM((GROUPS, late, half), BF16),
            pltpu.VMEM((GROUPS, late, half), BF16),
            pltpu.VMEM((tiles, 8, LANES), F32),
            pltpu.VMEM((tiles, users * capsules, LANES), BF16),
            pltpu.VMEM((4, tiles + 1, 8, LANES), F32),
            pltpu.VMEM((4, tiles + 1, 8, LANES), F32),
            pltpu.VMEM((8, LANES), F32),
            pltpu.VMEM((3, 8, LANES), F32),
            pltpu.VMEM((GROUPS, 1, LANES), jnp.int32),
            pltpu.VMEM((GROUPS, 1, LANES), jnp.int32),
            pltpu.VMEM((GROUPS, HOP, half), BF16),
            pltpu.VMEM((GROUPS, HOP, half), BF16),
            pltpu.VMEM((GROUPS * HOP, half), F32),
            pltpu.VMEM((GROUPS, SPILL, half), BF16),
            pltpu.VMEM((GROUPS, SPILL, half), BF16),
            pltpu.VMEM((GROUPS * SPILL, half), F32),
            dma((1,)), dma((1,)),
            dma((1,)), dma((2, CHUNKS)), dma((1,)), dma((CHUNKS,)),
            dma((1,)), dma((GROUPS // BATCH,)),
            dma((1,)), dma((4 * len(SPANS),)), dma((3,)), dma((3,)),
            dma((1,)), dma((1,)), dma((1,)), dma((1,)),
            dma((1,)), dma((1,)), dma((len(PHASES),)), dma((len(PHASES),)),
            pltpu.VMEM((GROUPS * HOP, rows_dev), BF16),
            *[pltpu.VMEM((GROUPS, size, half), BF16) for size in phases + phases],
        ],
        compiler_params=pltpu.CompilerParams(
            collective_id=collective_id, has_side_effects=True, vmem_limit_bytes=56 << 20
        ),
    )(item_ids, lengths, seed_rows, item_table, bilinear, seed_table)


def on_device(item_ids, lengths, seed_rows, item_table, bilinear, seed_table):
    maps = bilinear.reshape(COLS, -1, bilinear.shape[1])
    args = (item_ids, lengths, seed_rows, item_table, maps, seed_table.T)
    fast, fail = routed(64, 0, *args)
    return lax.cond(fail[0, 0] > 0, lambda: routed(LANES, 1, *args)[0], lambda: fast)


def solution(mesh):
    placed = (
        P("users", None),
        P("users"),
        P("users", None),
        P("users", "cols"),
        P(None, "cols"),
        P(),
    )
    return jax.shard_map(
        on_device, mesh=mesh, in_specs=placed, out_specs=P("users", None, "cols"), check_vma=False
    )
```
